256 devices in a mesh: unit: 2 (over core), block: 32 (over z, y), lane: 4 (over x).
Axes of the slice: x: 4, y: 4, z: 8, core: 2. Of those that a mesh axis runs over, the one named last changes fastest.
Arguments:
- image_rows: bfloat16 [16384, 512], P(('unit', 'block', 'lane')), parts along dimension 0, may hold values from -6 to 6, as said below
- text_rows: bfloat16 [16384, 512], P(('unit', 'block', 'lane')), parts along dimension 0, may hold values from -6 to 6, as said below
Outputs:
- image_loss: float32 [16384], P(('unit', 'block', 'lane')), parts along dimension 0
- text_loss: float32 [16384], P(('unit', 'block', 'lane')), parts along dimension 0
- image_grad: float32 [16384, 512], P(('unit', 'block', 'lane')), parts along dimension 0
- text_grad: float32 [16384, 512], P(('unit', 'block', 'lane')), parts along dimension 0
The draws below stay inside these ranges and needn't reach their ends.
There are 2 independent parts, one for each index of `unit`. The reference program is written for one: setup_inputs(seed, part) draws one part's arguments, and reference() takes and returns one part's arrays. A program takes and returns all parts, laid end to end along the dimension named above; each array names one. Nothing has to cross between parts.
Inputs may be any that keep to these rules, and one draw needn't show every extreme that they name: image_rows holds numbers from -6 to 6. text_rows holds numbers from -6 to 6.
All inputs are finite; a program needn't handle non-finite values.
Results may differ from the reference program's by a relative error of at most 0.0035.
Values may be sent and summed in bfloat16 or wider, within the bound.
A program may use at most 64 MiB of HBM per device.

```python
import jax
import jax.numpy as jnp
from jax import lax

EX_DEV = 64
EXAMPLES = 8192
EMBED = 512
DEVICES = 128


def shared_part(key):
    return jax.random.normal(jax.random.fold_in(key, 3), (EXAMPLES, EMBED), jnp.float32)


def one_tower(key, tag):
    own = jax.random.normal(jax.random.fold_in(key, tag), (EXAMPLES, EMBED), jnp.float32)
    group = jax.random.normal(jax.random.fold_in(key, 4), (DEVICES, 1, EMBED), jnp.float32)
    values = 0.6 * shared_part(key) + own
    values = values.reshape(DEVICES, EX_DEV, EMBED) + 0.7 * group
    return jnp.clip(values, -6.0, 6.0).reshape(EXAMPLES, EMBED).astype(jnp.bfloat16)


def draw_image_rows(key, part):
    return one_tower(key, 1)


def draw_text_rows(key, part):
    return one_tower(key, 2)


def setup_inputs(seed: int = 0, part: int = 0) -> dict:
    arg_keys = jax.random.split(jax.random.key(seed), 3)
    part_keys = jax.random.split(jax.random.fold_in(arg_keys[2], part), 3)
    return {
        "image_rows": draw_image_rows(jax.random.fold_in(jax.random.fold_in(arg_keys[2], part), 71), part),
        "text_rows": draw_text_rows(jax.random.fold_in(jax.random.fold_in(arg_keys[2], part), 71), part),
    }


def unit_rows(values):
    wide = values.astype(jnp.float32)
    return (wide * lax.rsqrt(lax.optimization_barrier(jnp.sum(wide * wide, axis=-1, keepdims=True)) + 1e-06)).astype(jnp.bfloat16)

def reference(image_rows, text_rows):
    image_unit, text_unit = lax.optimization_barrier((unit_rows(image_rows), unit_rows(text_rows)))
    blocks = image_unit.reshape(DEVICES, EX_DEV, EMBED)

    def block_sums(column_sum, block):
        power = jnp.exp(12.0 * jnp.dot(block, text_unit.T, preferred_element_type=jnp.float32))
        return (column_sum + lax.optimization_barrier(jnp.sum(power, axis=0)), lax.optimization_barrier(jnp.sum(power, axis=1)))
    column_sum, row_sum = lax.scan(block_sums, jnp.zeros((EXAMPLES,), jnp.float32), blocks)
    row_sum = row_sum.reshape(EXAMPLES)
    matched = 12.0 * lax.optimization_barrier(jnp.sum(image_unit.astype(jnp.float32) * text_unit.astype(jnp.float32), axis=1))
    image_loss, text_loss = (jnp.log(row_sum) - matched, jnp.log(column_sum) - matched)

    def block_grads(text_grad, item):
        block, sums, number = item
        power = jnp.exp(12.0 * jnp.dot(block, text_unit.T, preferred_element_type=jnp.float32))
        same = (number * EX_DEV + jnp.arange(EX_DEV))[:, None] == jnp.arange(EXAMPLES)[None, :]
        pull = (power / sums[:, None] + power / column_sum[None, :] - jnp.where(same, 2.0, 0.0)).astype(jnp.bfloat16)
        pull = lax.optimization_barrier(pull)
        image_part = jnp.dot(pull, text_unit, preferred_element_type=jnp.float32)
        return (text_grad + jnp.dot(pull.T, block, preferred_element_type=jnp.float32), image_part)
    text_grad, image_grad = lax.scan(block_grads, jnp.zeros((EXAMPLES, EMBED), jnp.float32), (blocks, row_sum.reshape(DEVICES, EX_DEV), jnp.arange(DEVICES)))
    image_grad = image_grad.reshape(EXAMPLES, EMBED)
    return (image_loss, text_loss, image_grad, text_grad)
```

```python
import functools

import jax
import jax.numpy as jnp
from jax import lax
from jax.experimental import pallas as pl
from jax.experimental.pallas import tpu as pltpu
from jax.sharding import PartitionSpec as P

NT = (((1,), (1,)), ((), ()))
F32, BF16 = jnp.float32, jnp.bfloat16

Z_SLOTS = [0, 1, 7, 2, 6, 3, 5, 4]
P_SLOTS = [
    (0, 0), (0, 1), (0, 3), (1, 0), (3, 0), (1, 1), (1, 3), (3, 1),
    (3, 3), (0, 2), (2, 0), (2, 1), (2, 3), (1, 2), (3, 2), (2, 2),
]
Z_NEAR = [2, 6, 1, 7]
Z_FAR = [(3, 0, 2, 2), (5, 0, 2, 6), (4, 0, 1, 2), (4, 1, 1, 6)]
P_NEAR = [(1, 1), (3, 3), (1, 3), (3, 1), (0, 1), (0, 3), (1, 0), (3, 0)]
P_FAR = [
    ((2, 2), 0, 1, (1, 1)), ((2, 2), 1, 1, (3, 3)),
    ((1, 2), 0, 1, (1, 1)), ((1, 2), 1, 1, (1, 3)),
    ((3, 2), 0, 1, (3, 1)), ((3, 2), 1, 1, (3, 3)),
    ((2, 1), 0, 1, (1, 1)), ((2, 1), 1, 1, (3, 1)),
    ((2, 3), 0, 1, (1, 3)), ((2, 3), 1, 1, (3, 3)),
    ((0, 2), 0, 1, (0, 1)), ((0, 2), 1, 1, (0, 3)),
    ((2, 0), 0, 1, (1, 0)), ((2, 0), 1, 1, (3, 0)),
]


class Ring:
    def __init__(self, size, here):
        self.size, self.here = size, here

    def neg(self, a):
        return -a % self.size

    def sub(self, a, b):
        return (a - b) % self.size

    def index(self, a):
        return lax.rem(self.here + a, self.size)


class Line:
    slots, near, far = Z_SLOTS, Z_NEAR, Z_FAR

    def __init__(self, side, z, y):
        self.z, self.y, self.side = Ring(8, z), y, side

    def neg(self, a):
        return self.z.neg(a)

    def sub(self, a, b):
        return self.z.sub(a, b)

    def device(self, a):
        return {"block": self.z.index(a) * self.side + self.y}

    def index(self, a):
        return self.z.index(a)


class Plane:
    slots, near, far = P_SLOTS, P_NEAR, P_FAR

    def __init__(self, side, z, y, x):
        self.z, self.y, self.x, self.side = z, Ring(side, y), Ring(side, x), side

    def neg(self, a):
        return (self.y.neg(a[0]), self.x.neg(a[1]))

    def sub(self, a, b):
        return (self.y.sub(a[0], b[0]), self.x.sub(a[1], b[1]))

    def device(self, a):
        return {"block": self.z * self.side + self.y.index(a[0]), "lane": self.x.index(a[1])}

    def index(self, a):
        return self.y.index(a[0]) * self.side + self.x.index(a[1])


def unit_rows(values):
    wide = values.astype(F32)
    scale = lax.rsqrt(jnp.sum(wide * wide, axis=-1, keepdims=True) + 1e-06)
    return (wide * scale).astype(BF16)


def upright(row):
    return jnp.transpose(jnp.broadcast_to(row, (8, row.shape[1])))[:, :1]


class Side:
    def __init__(self, group, rows, data, sums, mine, own, out, far_in, near_in, sems):
        self.g, self.rows, self.data, self.sums, self.mine = group, rows, data, sums, mine
        self.own, self.out, self.far_in, self.near_in = own, out, far_in, near_in
        self.pos = {slot: k for k, slot in enumerate(group.slots)}
        ag1, ag2, sm, rs1, rs2 = [(sems[2 * k], sems[2 * k + 1]) for k in range(5)]
        g = group

        def remote(src, dst, sem, k, offset):
            return pltpu.make_async_remote_copy(
                src_ref=src, dst_ref=dst, send_sem=sem[0].at[k], recv_sem=sem[1].at[k],
                device_id=g.device(offset),
            )

        self.gather_near = {
            o: remote(data.at[self.rows_of(g.slots[0])], data.at[self.rows_of(g.neg(o))], ag1, k, o)
            for k, o in enumerate(g.near)
        }
        self.gather_far = [
            remote(
                data.at[self.rows_of(g.neg(r), h, n)], data.at[self.rows_of(g.neg(o), h, n)],
                ag2, k, g.sub(o, r),
            )
            for k, (o, h, n, r) in enumerate(g.far)
        ]
        self.exchange = [
            remote(mine, sums.at[k], sm, k, o) for k, o in enumerate(g.slots[1:])
        ]
        self.reduce_far = [
            remote(
                out.at[self.rows_of(g.neg(o), h, n)], far_in.at[k, pl.ds(0, n * rows // 2)],
                rs1, k, g.sub(r, o),
            )
            for k, (o, h, n, r) in enumerate(g.far)
        ]
        self.reduce_near = {
            o: remote(out.at[self.rows_of(g.neg(o))], near_in.at[k], rs2, k, g.neg(o))
            for k, o in enumerate(g.near)
        }

    def rows_of(self, slot, half=0, halves=2):
        return pl.ds(self.pos[slot] * self.rows + half * self.rows // 2, halves * self.rows // 2)

    def start_gather(self):
        for o in self.g.near:
            self.gather_near[o].start()

    def relay_gather(self):
        for o in self.g.near:
            self.gather_near[o].wait_recv()
            for k, (_, _, _, r) in enumerate(self.g.far):
                if r == o:
                    self.gather_far[k].start()

    def finish_gather(self, slots):
        for k, (o, _, _, _) in enumerate(self.g.far):
            if self.g.neg(o) in slots:
                self.gather_far[k].wait_recv()

    def keep_sum(self, position, row):
        slot = self.g.slots[position]
        self.mine[pl.ds(self.g.index(slot), 1), 0 : self.rows] = row

    def start_sums(self):
        for copy in self.exchange:
            copy.start()

    def total(self):
        for copy in self.exchange:
            copy.wait_recv()
        total = self.mine[...]
        for k in range(len(self.exchange)):
            total = total + self.sums[k]
        return total

    def send_far(self, slots):
        for k, (o, _, _, _) in enumerate(self.g.far):
            if self.g.neg(o) in slots:
                self.reduce_far[k].start()

    def send_near(self, o):
        where = self.rows_of(self.g.neg(o))
        added = False
        for k, (_, h, n, r) in enumerate(self.g.far):
            if r == o:
                self.reduce_far[k].wait_recv()
                part = self.rows_of(self.g.neg(o), h, n)
                self.own[part, :] += self.far_in[k, pl.ds(0, n * self.rows // 2)].astype(F32)
                added = True
        if added:
            self.out[where, :] = self.own[where, :].astype(BF16)
        self.reduce_near[o].start()

    def gradient(self):
        for o in self.g.near:
            self.reduce_near[o].wait_recv()
        grad = self.own[self.rows_of(self.g.slots[0]), :]
        for k in range(len(self.g.near)):
            grad = grad + self.near_in[k].astype(F32)
        return grad

    def wait_sends(self):
        for copies in (
            list(self.gather_near.values()), self.gather_far, self.exchange,
            self.reduce_far, list(self.reduce_near.values()),
        ):
            for copy in copies:
                copy.wait_send()


def kernel(
    side, group,
    image_hbm, text_hbm,
    image_loss, text_loss, image_grad, text_grad,
    image_raw, text_raw, images, texts, power, power_t,
    row_mine, row_in, col_mine, col_in, row_tot, col_tot, row_all, col_all,
    image_own, text_own, image_out, text_out,
    image_far, text_far, image_near, text_near,
    load_sem, *sems,
):
    lane, block = lax.axis_index("lane"), lax.axis_index("block")
    z, y = block // side, lax.rem(block, side)
    rows = image_raw.shape[0]
    per = group // rows
    image = Side(Line(side, z, y), rows, images, row_in, row_mine, image_own, image_out, image_far, image_near, sems[:10])
    text = Side(Plane(side, z, y, lane), rows, texts, col_in, col_mine, text_own, text_out, text_far, text_near, sems[10:])
    image_groups, text_groups = len(Z_SLOTS) // per, len(P_SLOTS) // per

    loads = [
        pltpu.make_async_copy(image_hbm, image_raw, load_sem.at[0]),
        pltpu.make_async_copy(text_hbm, text_raw, load_sem.at[1]),
    ]
    for load in loads:
        load.start()
    barrier = pltpu.get_barrier_semaphore()
    for part in (image, text):
        for o in part.g.near:
            pl.semaphore_signal(barrier, inc=1, device_id=part.g.device(o))

    loads[1].wait()
    texts[0:rows, :] = unit_rows(text_raw[...])
    loads[0].wait()
    images[0:rows, :] = unit_rows(image_raw[...])
    pl.semaphore_wait(barrier, len(Z_NEAR) + len(P_NEAR))
    text.start_gather()
    image.start_gather()

    pair = 12.0 * lax.dot_general(images[0:rows, :], texts[0:rows, :], NT, preferred_element_type=F32)
    eye = lax.broadcasted_iota(jnp.int32, (rows, rows), 0) == lax.broadcasted_iota(jnp.int32, (rows, rows), 1)
    matched = jnp.sum(jnp.where(eye, pair, 0.0), axis=0, keepdims=True)

    image.relay_gather()
    text.relay_gather()

    def some(g):
        return pl.ds(g * group, group)

    row_sums, col_sums = [0.0] * image_groups, [0.0] * text_groups

    def powers(h, g):
        i, t = images[some(h), :], texts[some(g), :]
        p = jnp.exp(12.0 * lax.dot_general(i, t, NT, preferred_element_type=F32))
        q = jnp.exp(12.0 * lax.dot_general(t, i, NT, preferred_element_type=F32))
        power[some(h), some(g)] = p
        power_t[some(g), some(h)] = q
        col_sums[g] += jnp.sum(p, axis=0, keepdims=True)
        row_sums[h] += jnp.sum(q, axis=0, keepdims=True)

    powers(0, 0)
    powers(0, 1)
    image.finish_gather(Z_SLOTS)
    powers(1, 0)
    powers(1, 1)
    text.finish_gather(P_SLOTS[2 * per : 3 * per])
    powers(0, 2)
    powers(1, 2)
    text.finish_gather(P_SLOTS[3 * per :])
    powers(0, 3)
    powers(1, 3)

    for part, sums in ((image, row_sums), (text, col_sums)):
        for g, row in enumerate(sums):
            for k in range(per):
                part.keep_sum(g * per + k, row[:, k * rows : (k + 1) * rows])
        part.start_sums()

    def inverse(part, totals, lines):
        totals[...] = 1.0 / part.total()
        for k, slot in enumerate(part.g.slots):
            lines[:, k * rows : (k + 1) * rows] = totals[pl.ds(part.g.index(slot), 1), 0:rows]

    inverse(image, row_tot, row_all)
    inverse(text, col_tot, col_all)
    row_inv, col_inv = row_all[...], col_all[...]
    row_inv_up, col_inv_up = upright(row_inv), upright(col_inv)
    image_loss[...] = -jnp.log(row_inv[:, 0:rows]) - matched
    text_loss[...] = -jnp.log(col_inv[:, 0:rows]) - matched

    def own_two(values):
        ids = [lax.broadcasted_iota(jnp.int32, values.shape, d) for d in (0, 1)]
        return values - jnp.where((ids[0] == ids[1]) & (ids[0] < rows), 2.0, 0.0)

    def text_part(g):
        here = some(g)
        pull = power_t[here, :] * (row_inv + col_inv_up[g * group : (g + 1) * group])
        pull = (own_two(pull) if g == 0 else pull).astype(BF16)
        part = jnp.dot(pull, images[...], preferred_element_type=F32)
        text_own[here, :] = part
        text_out[here, :] = part.astype(BF16)
        text.send_far(P_SLOTS[g * per : (g + 1) * per])

    def image_part(h):
        here = some(h)
        pull = power[here, :] * (row_inv_up[h * group : (h + 1) * group] + col_inv)
        pull = (own_two(pull) if h == 0 else pull).astype(BF16)
        part = jnp.dot(pull, texts[...], preferred_element_type=F32)
        image_own[here, :] = part
        image_out[here, :] = part.astype(BF16)
        image.send_far(Z_SLOTS[h * per : (h + 1) * per])

    text_part(3)
    image_part(1)
    text_part(2)
    text_part(1)
    image_part(0)
    for o in (1, 7, 2, 6):
        image.send_near(o)
    text_part(0)
    for o in P_NEAR:
        text.send_near(o)
    image_grad[...] = image.gradient()
    text_grad[...] = text.gradient()
    image.wait_sends()
    text.wait_sends()


def place(*refs):
    sem = refs[-1]
    copies = [
        pltpu.make_async_copy(refs[i], refs[i + 4], sem.at[i]) for i in (2, 3, 0, 1)
    ]
    for copy in copies:
        copy.start()
    for copy in copies:
        copy.wait()


def solution(mesh):
    side = mesh.shape["lane"]

    def body(image_rows, text_rows):
        rows, width = image_rows.shape
        nz, npl = len(Z_SLOTS), len(P_SLOTS)
        images_n, texts_n = nz * rows, npl * rows
        group = 4 * rows
        scratch = [
            pltpu.VMEM((rows, width), BF16),
            pltpu.VMEM((rows, width), BF16),
            pltpu.VMEM((images_n, width), BF16),
            pltpu.VMEM((texts_n, width), BF16),
            pltpu.VMEM((images_n, texts_n), F32),
            pltpu.VMEM((texts_n, images_n), F32),
            pltpu.VMEM((nz, 128), F32),
            pltpu.VMEM((nz - 1, nz, 128), F32),
            pltpu.VMEM((npl, 128), F32),
            pltpu.VMEM((npl - 1, npl, 128), F32),
            pltpu.VMEM((nz, 128), F32),
            pltpu.VMEM((npl, 128), F32),
            pltpu.VMEM((1, images_n), F32),
            pltpu.VMEM((1, texts_n), F32),
            pltpu.VMEM((images_n, width), F32),
            pltpu.VMEM((texts_n, width), F32),
            pltpu.VMEM((images_n, width), BF16),
            pltpu.VMEM((texts_n, width), BF16),
            pltpu.VMEM((len(Z_FAR), rows, width), BF16),
            pltpu.VMEM((len(P_FAR), rows // 2, width), BF16),
            pltpu.VMEM((len(Z_NEAR), rows, width), BF16),
            pltpu.VMEM((len(P_NEAR), rows, width), BF16),
            pltpu.SemaphoreType.DMA((2,)),
        ]
        for near, far, all_ in ((len(Z_NEAR), len(Z_FAR), nz), (len(P_NEAR), len(P_FAR), npl)):
            for count in (near, far, all_ - 1, far, near):
                scratch += [pltpu.SemaphoreType.DMA((count,))] * 2
        results = pl.pallas_call(
            functools.partial(kernel, side, group),
            out_shape=(
                jax.ShapeDtypeStruct((1, rows), F32),
                jax.ShapeDtypeStruct((1, rows), F32),
                jax.ShapeDtypeStruct((rows, width), F32),
                jax.ShapeDtypeStruct((rows, width), F32),
            ),
            in_specs=[pl.BlockSpec(memory_space=pltpu.HBM)] * 2,
            out_specs=[pl.BlockSpec(memory_space=pltpu.VMEM)] * 4,
            scratch_shapes=scratch,
            compiler_params=pltpu.CompilerParams(
                collective_id=0, has_side_effects=True, vmem_limit_bytes=40 * 2**20
            ),
        )(*(pltpu.with_memory_space_constraint(x, pltpu.HBM) for x in (image_rows, text_rows)))
        image_loss, text_loss, image_grad, text_grad = pl.pallas_call(
            place,
            out_shape=tuple(jax.ShapeDtypeStruct(r.shape, r.dtype) for r in results),
            in_specs=[pl.BlockSpec(memory_space=pltpu.VMEM)] * 4,
            out_specs=[pl.BlockSpec(memory_space=pl.ANY)] * 4,
            scratch_shapes=[pltpu.SemaphoreType.DMA((4,))],
            compiler_params=pltpu.CompilerParams(vmem_limit_bytes=4 * rows * width * 8),
        )(*results)
        return (image_loss.reshape(rows), text_loss.reshape(rows), image_grad, text_grad)

    rows_spec = P(("unit", "block", "lane"), None)
    flat_spec = P(("unit", "block", "lane"))
    return jax.shard_map(
        body,
        mesh=mesh,
        in_specs=(rows_spec, rows_spec),
        out_specs=(flat_spec, flat_spec, rows_spec, rows_spec),
        check_vma=False,
    )
```

```python
import functools

import jax
import jax.numpy as jnp
from jax import lax
from jax.experimental import pallas as pl
from jax.experimental.pallas import tpu as pltpu
from jax.sharding import PartitionSpec as P

NT = (((1,), (1,)), ((), ()))
TN = (((0,), (0,)), ((), ()))
LOG2E = 1.4426950408889634
F32, BF16 = jnp.float32, jnp.bfloat16
PIECES = 2
RECV_SEMS = (12, 22)
BACK_ORDER = [(1, 12, 16), (0, 4, 8), (1, 8, 12), (0, 0, 4), (1, 4, 8), (1, 0, 4)]
IMAGE_GROUPS, TEXT_GROUPS = (4, 4), (4, 4, 8)

PLANS = [
    (
        (
            [
                ((4,), 1, (2,), 10.8), ((2,), 0, (1,), 6.9), ((3,), 0, (1,), 8.2), ((3,), 1, (1,), 9.5),
                ((6,), 0, (0,), 5.8), ((2,), 1, (0,), 5.8), ((7,), 1, (0,), 3.4), ((7,), 0, (0,), 4.1),
                ((6,), 1, (7,), 6.9), ((1,), 0, (0,), 3.4), ((5,), 0, (7,), 9.5), ((4,), 0, (6,), 10.8),
                ((1,), 1, (0,), 4.1), ((5,), 1, (7,), 8.2),
            ],
            [
                ((5,), 0, (6,), 4.3), ((1,), 0, (0,), 6.9), ((2,), 1, (0,), 8.8), ((6,), 0, (0,), 8.8),
                ((1,), 1, (0,), 7.5), ((3,), 1, (2,), 4.3), ((7,), 1, (0,), 6.9), ((5,), 1, (6,), 4.9),
                ((7,), 0, (0,), 7.5), ((6,), 1, (0,), 10.4), ((3,), 0, (2,), 4.9), ((4,), 0, (2,), 6.2),
                ((2,), 0, (0,), 10.4), ((4,), 1, (6,), 6.2),
            ],
        ),
        (
            [
                ((3, 2), 0, (3, 3), 10.8), ((2, 0), 1, (3, 0), 7.0), ((2, 3), 0, (1, 3), 10.3), ((1, 0), 0, (0, 0), 3.4),
                ((1, 1), 1, (0, 1), 7.0), ((0, 2), 0, (0, 3), 6.9), ((3, 0), 1, (0, 0), 3.4), ((0, 1), 1, (0, 0), 3.4),
                ((2, 2), 0, (1, 3), 10.9), ((0, 3), 0, (0, 0), 3.4), ((3, 1), 1, (0, 0), 5.7), ((1, 0), 1, (0, 0), 4.1),
                ((1, 3), 0, (0, 0), 5.7), ((3, 3), 1, (3, 0), 7.6), ((1, 1), 0, (0, 0), 6.4), ((3, 0), 0, (0, 0), 4.1),
                ((2, 2), 1, (3, 1), 10.1), ((1, 3), 1, (0, 3), 8.3), ((2, 1), 0, (3, 0), 8.8), ((2, 0), 0, (1, 0), 7.7),
                ((2, 1), 1, (3, 0), 7.7), ((0, 1), 0, (0, 0), 4.1), ((0, 2), 1, (0, 1), 7.6), ((3, 1), 0, (3, 0), 8.9),
                ((1, 2), 0, (1, 3), 10.2), ((3, 3), 0, (0, 0), 6.4), ((0, 3), 1, (0, 0), 4.1), ((1, 2), 1, (0, 3), 9.0),
                ((3, 2), 1, (3, 1), 10.2), ((2, 3), 1, (1, 0), 9.6),
            ],
            [
                ((3, 0), 0, (0, 0), 7.2), ((1, 0), 1, (0, 0), 7.8), ((2, 1), 1, (3, 1), 5.2), ((0, 3), 0, (0, 0), 10.7),
                ((2, 3), 1, (1, 3), 3.9), ((3, 1), 0, (0, 1), 5.9), ((2, 2), 1, (1, 3), 4.6), ((1, 1), 1, (0, 0), 8.6),
                ((3, 1), 1, (0, 0), 9.3), ((1, 2), 0, (1, 3), 4.6), ((2, 0), 0, (1, 0), 6.5), ((1, 3), 0, (0, 0), 9.9),
                ((0, 2), 1, (0, 1), 6.5), ((2, 3), 0, (3, 3), 3.9), ((3, 2), 0, (0, 1), 4.6), ((3, 0), 1, (0, 0), 10.0),
                ((1, 1), 0, (1, 0), 7.2), ((0, 3), 1, (0, 0), 5.9), ((2, 2), 0, (1, 3), 5.8), ((1, 2), 1, (1, 1), 4.6),
                ((3, 2), 1, (3, 1), 5.2), ((0, 1), 0, (0, 0), 9.4), ((3, 3), 1, (3, 0), 6.5), ((1, 0), 0, (0, 0), 10.7),
                ((2, 0), 1, (3, 0), 6.5), ((1, 3), 1, (0, 0), 9.3), ((0, 2), 0, (0, 3), 7.2), ((3, 3), 0, (0, 0), 8.4),
                ((2, 1), 0, (1, 0), 7.1), ((0, 1), 1, (0, 0), 10.0),
            ],
        ),
    ),
    (
        (
            [
                ((5,), 1, (6,), 7.1), ((6,), 1, (0,), 4.5), ((5,), 0, (7,), 5.8), ((7,), 0, (0,), 2.4),
                ((4,), 0, (5,), 8.3), ((6,), 0, (7,), 6.4), ((1,), 1, (0,), 2.4), ((2,), 0, (0,), 4.5),
                ((7,), 1, (0,), 3.1), ((3,), 1, (1,), 5.8), ((2,), 1, (1,), 6.4), ((3,), 0, (2,), 7.1),
                ((1,), 0, (0,), 3.1), ((4,), 1, (3,), 8.3),
            ],
            [
                ((7,), 0, (0,), 4.6), ((1,), 1, (0,), 4.6), ((2,), 0, (0,), 9.0), ((3,), 0, (2,), 5.9),
                ((4,), 0, (3,), 3.3), ((3,), 1, (2,), 3.9), ((1,), 0, (0,), 5.2), ((5,), 1, (6,), 5.9),
                ((2,), 1, (0,), 7.2), ((6,), 1, (0,), 9.0), ((4,), 1, (5,), 3.3), ((6,), 0, (0,), 7.2),
                ((5,), 0, (6,), 3.9), ((7,), 1, (0,), 5.2),
            ],
        ),
        (
            [
                ((1, 2), 1, (1, 1), 8.0), ((1, 1), 1, (0, 1), 5.1), ((2, 2), 1, (2, 3), 8.6), ((2, 3), 1, (1, 0), 6.1),
                ((1, 0), 0, (0, 0), 2.4), ((3, 0), 1, (0, 0), 2.4), ((3, 1), 1, (0, 0), 4.4), ((3, 0), 0, (0, 0), 3.1),
                ((0, 3), 0, (0, 0), 2.4), ((1, 1), 0, (1, 0), 4.9), ((0, 2), 1, (0, 3), 6.2), ((1, 2), 0, (1, 1), 7.4),
                ((3, 3), 0, (0, 3), 5.1), ((0, 1), 1, (0, 0), 2.4), ((3, 3), 1, (3, 0), 4.9), ((2, 1), 1, (3, 1), 7.0),
                ((3, 2), 1, (3, 3), 7.5), ((2, 0), 0, (3, 0), 6.4), ((2, 1), 0, (1, 1), 8.1), ((1, 3), 0, (0, 0), 4.4),
                ((2, 3), 0, (3, 3), 7.7), ((3, 1), 0, (3, 0), 5.6), ((1, 3), 1, (0, 3), 6.8), ((2, 2), 0, (1, 3), 7.5),
                ((2, 0), 1, (3, 0), 5.7), ((0, 3), 1, (0, 0), 3.1), ((1, 0), 1, (0, 0), 3.1), ((0, 1), 0, (0, 0), 3.1),
                ((0, 2), 0, (0, 1), 6.2), ((3, 2), 0, (0, 2), 8.7),
            ],
            [
                ((0, 3), 0, (0, 0), 6.8), ((2, 2), 1, (1, 2), 2.9), ((0, 2), 0, (0, 1), 4.9), ((1, 1), 0, (0, 1), 4.9),
                ((1, 1), 1, (0, 1), 5.5), ((1, 3), 1, (1, 0), 3.6), ((2, 0), 1, (3, 0), 4.9), ((2, 0), 0, (1, 0), 3.6),
                ((1, 3), 0, (0, 0), 8.1), ((3, 2), 1, (3, 1), 2.9), ((3, 1), 0, (0, 0), 7.3), ((3, 3), 0, (3, 0), 5.5),
                ((2, 1), 0, (3, 1), 2.9), ((0, 1), 0, (0, 0), 7.4), ((0, 3), 1, (0, 0), 8.1), ((0, 1), 1, (0, 0), 8.7),
                ((0, 2), 1, (0, 3), 4.2), ((2, 3), 0, (1, 3), 4.2), ((3, 1), 1, (0, 1), 6.2), ((1, 0), 0, (0, 0), 6.8),
                ((2, 1), 1, (3, 1), 3.6), ((2, 2), 0, (3, 1), 4.2), ((1, 0), 1, (0, 0), 7.5), ((1, 2), 0, (1, 3), 2.9),
                ((1, 2), 1, (0, 1), 6.2), ((3, 2), 0, (3, 1), 4.2), ((3, 3), 1, (3, 0), 6.2), ((2, 3), 1, (3, 0), 5.5),
                ((3, 0), 0, (0, 0), 8.0), ((3, 0), 1, (0, 0), 8.7),
            ],
        ),
    ),
]


def rectangles(cells):
    found = []
    for h in sorted({h for h, _ in cells}):
        runs = []
        for g in sorted(g for k, g in cells if k == h):
            if runs and runs[-1][-1] == g - 1:
                runs[-1].append(g)
            else:
                runs.append([g])
        for run in runs:
            match = [hs for hs, gs in found if gs == run and hs[-1] == h - 1]
            if match:
                match[0].append(h)
            else:
                found.append(([h], run))
    return found


class Group:
    def __init__(self, route, sizes, here, device):
        self.sizes, self.here, self.device_of = sizes, here, device
        self.home = (0,) * len(sizes)
        when = {self.home: 0.0}
        for o, _, _, t in route:
            when[self.neg(o)] = max(t, when.get(self.neg(o), 0.0))
        self.slots = sorted(when, key=when.get)

    def sub(self, a, b):
        return tuple((i - j) % n for i, j, n in zip(a, b, self.sizes))

    def neg(self, a):
        return tuple(-i % n for i, n in zip(a, self.sizes))

    def at(self, a):
        return [lax.rem(h + i, n) if i else h for h, i, n in zip(self.here, a, self.sizes)]

    def device(self, a):
        return self.device_of(*self.at(a))

    def index(self, a):
        index = 0
        for i, n in zip(self.at(a), self.sizes):
            index = index * n + i
        return index


def unit_rows(values):
    wide = values.astype(F32)
    scale = lax.rsqrt(jnp.sum(wide * wide, axis=-1, keepdims=True) + 1e-06)
    return (wide * scale).astype(BF16)


def upright(row):
    return jnp.transpose(jnp.broadcast_to(row, (8, row.shape[1])))[:, :1]


class Side:
    def __init__(self, group, group_of, routes, rows, data, sums, mine, own, out, inbox, sems):
        self.g, self.rows, self.data, self.sums, self.mine = group, rows, data, sums, mine
        self.out_route, self.back_route = routes
        self.own, self.out, self.inbox = own, out, inbox
        self.send, self.recv, self.sum_recv = sems
        self.pos = {slot: k for k, slot in enumerate(group.slots)}
        self.home = group.home
        self.landed = set()
        g = group

        def remote(send, src, dst, recv, offset):
            return pltpu.make_async_remote_copy(
                src_ref=src, dst_ref=dst, send_sem=self.send.at[send], recv_sem=recv, device_id=g.device(offset)
            )

        self.out_pools, self.back_pools = self.pools(group_of)
        assert max(len(self.out_pools), len(self.back_pools)) <= self.recv.shape[0]
        out_pool, back_pool = ({k: n for n, ks in enumerate(pools) for k in ks} for pools in (self.out_pools, self.back_pools))
        self.gather = [
            remote(
                0, data.at[self.piece(g.neg(r), p)], data.at[self.piece(g.neg(o), p)],
                self.recv.at[out_pool[k]], g.sub(o, r),
            )
            for k, (o, p, r, _) in enumerate(self.out_route)
        ]
        self.exchange = [
            remote(1, mine, sums.at[k], self.sum_recv.at[0], o) for k, o in enumerate(reversed(g.slots[1:]))
        ]
        self.reduce = [
            remote(0, out.at[self.piece(g.neg(o), p)], inbox.at[k], self.recv.at[back_pool[k]], g.sub(r, o))
            for k, (o, p, r, _) in enumerate(self.back_route)
        ]

    def pools(self, group_of):
        out, back = {}, {}
        for k, (o, p, _, _) in enumerate(self.out_route):
            out.setdefault(("at", k) if self.onward(o, p) else ("of", group_of[self.pos[self.g.neg(o)]]), []).append(k)
        for k, (_, p, r, _) in enumerate(self.back_route):
            if r != self.home:
                back.setdefault((r, p), []).append(k)
        home = [k for _, k in sorted(self.home_parts())]
        while home:
            count = min(4, max(1, len(home) // 2))
            back[home[0]], home = home[:count], home[count:]
        return list(out.values()), list(back.values())

    def wait_pool(self, pools, n):
        amount = self.inbox.at[pl.ds(0, len(pools[n]))]
        pltpu.make_async_copy(amount, amount, self.recv.at[n]).wait()

    def hops(self, offset):
        return sum(min(i, n - i) for i, n in zip(offset, self.g.sizes))

    def next_to(self):
        return [o for o in self.g.slots if self.hops(o) == 1]

    def piece(self, slot, p):
        size = self.rows // PIECES
        return pl.ds(self.pos[slot] * self.rows + p * size, size)

    def onward(self, o, p):
        return [k for k, (_, q, r, _) in enumerate(self.out_route) if r == o and q == p]

    def inward(self, o, p):
        parts = [(t, k) for k, (_, q, r, t) in enumerate(self.back_route) if r == o and q == p]
        return [k for _, k in sorted(parts)]

    def start_gather(self, hops):
        for k, (o, _, r, _) in enumerate(self.out_route):
            if r == self.home and self.hops(o) == hops:
                self.gather[k].start()

    def arrive(self, k):
        o, p, _, _ = self.out_route[k]
        pool = [n for n, ks in enumerate(self.out_pools) if k in ks][0]
        self.landed.add(k)
        if not self.landed.issuperset(self.out_pools[pool]):
            return
        self.wait_pool(self.out_pools, pool)
        for j in self.onward(o, p):
            assert self.hops(self.g.sub(self.out_route[j][0], o)) <= 2
            self.gather[j].start()

    def keep_sum(self, position, row):
        slot = self.g.slots[position]
        self.mine[pl.ds(self.g.index(slot), 1), 0 : self.rows] = row

    def start_sums(self):
        for copy in self.exchange:
            copy.start()

    def total(self):
        pltpu.make_async_copy(self.sums, self.sums, self.sum_recv.at[0]).wait()
        total = self.mine[...]
        for k in range(len(self.exchange)):
            total = total + self.sums[k]
        return total

    def send_ready(self, slots):
        for k, (o, p, _, _) in enumerate(self.back_route):
            if self.g.neg(o) in slots and not self.inward(o, p):
                self.reduce[k].start()

    def stops(self):
        parts = [(self.inward(o, p), k) for k, (o, p, _, _) in enumerate(self.back_route)]
        return [(self.back_route[inward[-1]][3], k) for inward, k in parts if inward]

    def pass_on(self, k):
        o, p, _, _ = self.back_route[k]
        where = self.piece(self.g.neg(o), p)
        total = self.own[where, :]
        parts = self.inward(o, p)
        self.wait_pool(self.back_pools, [n for n, ks in enumerate(self.back_pools) if parts[0] in ks][0])
        for j in parts:
            total = total + self.inbox[j].astype(F32)
        self.out[where, :] = total.astype(BF16)
        self.reduce[k].start()

    def home_parts(self):
        return [(t, k) for k, (_, _, r, t) in enumerate(self.back_route) if r == self.home]

    def home_pools(self):
        when = dict((k, t) for t, k in self.home_parts())
        return [(max(when[k] for k in ks), n) for n, ks in enumerate(self.back_pools) if ks[0] in when]

    def add_home(self, n, grad):
        size = self.rows // PIECES
        self.wait_pool(self.back_pools, n)
        for p in range(PIECES):
            parts = [k for k in self.back_pools[n] if self.back_route[k][1] == p]
            if parts:
                here = slice(p * size, (p + 1) * size)
                grad[here, :] = sum((self.inbox[k].astype(F32) for k in parts), grad[here, :])

    def wait_sends(self, n):
        amount = (self.inbox, self.sums)[n]
        pltpu.make_async_copy(amount, amount, self.send.at[n]).wait()


def kernel(
    side,
    image_hbm, text_hbm,
    image_loss, text_loss, image_grad, text_grad,
    image_raw, text_raw, images, texts, power, pull,
    row_mine, row_in, col_mine, col_in, row_tot, col_tot, row_all, col_all,
    image_own, text_own, image_out, text_out, image_box, text_box,
    around, *sems,
):
    lane, block, unit = lax.axis_index("lane"), lax.axis_index("block"), lax.axis_index("unit")
    z, y = block // side, lax.rem(block, side)
    rows = image_raw.shape[0]
    image_count = row_mine.shape[0]
    sizes = (IMAGE_GROUPS, TEXT_GROUPS)
    first = [[sum(s[:g]) for g in range(len(s) + 1)] for s in sizes]
    group_of = [[g for g, n in enumerate(s) for _ in range(n)] for s in sizes]

    loads = [
        pltpu.make_async_copy(image_hbm, image_raw, sems[0].at[0]),
        pltpu.make_async_copy(text_hbm, text_raw, sems[3].at[0]),
    ]
    for load in loads:
        load.start()
    barrier = pltpu.get_barrier_semaphore()

    def sides(plan):
        line = Group(plan[0][0], (image_count,), (z,), lambda k: {"block": k * side + y})
        plane = Group(plan[1][0], (side, side), (y, lane), lambda k, j: {"block": z * side + k, "lane": j})
        return (
            Side(line, group_of[0], plan[0], rows, images, row_in, row_mine, image_own, image_out, image_box, sems[:3]),
            Side(plane, group_of[1], plan[1], rows, texts, col_in, col_mine, text_own, text_out, text_box, sems[3:]),
        )

    def some(s, gs):
        start, end = first[s][gs[0]] * rows, first[s][gs[-1] + 1] * rows
        return pl.ds(start, end - start)

    def run(plan):
        image, text = sides(plan)
        for part in (image, text):
            for o in part.next_to():
                pl.semaphore_signal(barrier, inc=1, device_id=part.g.device(o))
        with jax.named_scope("load"):
            loads[1].wait()
            texts[0:rows, :] = unit_rows(text_raw[...])
            loads[0].wait()
            images[0:rows, :] = unit_rows(image_raw[...])
        with jax.named_scope("barrier"):
            pl.semaphore_wait(barrier, len(image.next_to()) + len(text.next_to()))
        for part in (image, text):
            for o in part.next_to():
                pl.semaphore_signal(around, inc=1, device_id=part.g.device(o))
        text.start_gather(1)
        image.start_gather(1)

        pair = 12.0 * lax.dot_general(images[0:rows, :], texts[0:rows, :], NT, preferred_element_type=F32)
        eye = lax.broadcasted_iota(jnp.int32, (rows, rows), 0) == lax.broadcasted_iota(jnp.int32, (rows, rows), 1)
        matched = jnp.sum(jnp.where(eye, pair, 0.0), axis=0, keepdims=True)

        with jax.named_scope("around"):
            pl.semaphore_wait(around, len(image.next_to()) + len(text.next_to()))
        text.start_gather(2)
        image.start_gather(2)

        row_sums, col_sums = [0.0] * len(IMAGE_GROUPS), [0.0] * len(TEXT_GROUPS)

        def powers(hs, gs):
            here, there = some(0, hs), some(1, gs)
            logit = lax.dot_general(images[here, :], texts[there, :], NT, preferred_element_type=F32)
            p = jnp.exp2((12.0 * LOG2E) * logit)
            power[here, there] = p
            lanes = sum(p[:, k : k + 128] for k in range(0, p.shape[1], 128))
            for s, groups, sums in ((0, hs, row_sums), (1, gs, col_sums)):
                start = 0
                for g in groups:
                    end = start + sizes[s][g] * rows
                    sums[g] += jnp.sum(p[:, start:end], axis=0, keepdims=True) if s else lanes[start:end]
                    start = end

        waits = sorted(
            (t, s, k) for s, part in enumerate((image, text)) for k, (_, _, _, t) in enumerate(part.out_route)
        )
        missing = {(s, g): set() for s in (0, 1) for g in range(len(sizes[s]))}
        for s, part in enumerate((image, text)):
            for k, (o, _, _, _) in enumerate(part.out_route):
                missing[(s, group_of[s][part.pos[part.g.neg(o)]])].add(k)
        todo = {(h, g) for h in range(len(IMAGE_GROUPS)) for g in range(len(TEXT_GROUPS))}
        for _, s, k in waits:
            part = (image, text)[s]
            with jax.named_scope(f"arrive_{'it'[s]}{k:02d}"):
                part.arrive(k)
            missing[(s, group_of[s][part.pos[part.g.neg(part.out_route[k][0])]])].discard(k)
            ready = {(h, g) for h, g in todo if not missing[(0, h)] and not missing[(1, g)]}
            todo -= ready
            for hs, gs in rectangles(ready):
                with jax.named_scope(f"pow{hs[0]}{gs[0]}"):
                    powers(hs, gs)

        with jax.named_scope("sums_out"):
            for s, part, sums in ((1, text, col_sums), (0, image, row_sums)):
                for g, row in enumerate(sums):
                    row = row if s else jnp.sum(jnp.transpose(row), axis=0, keepdims=True)
                    for k in range(sizes[s][g]):
                        part.keep_sum(first[s][g] + k, row[:, k * rows : (k + 1) * rows])
                part.start_sums()

        def inverse(part, totals, lines):
            totals[...] = 1.0 / part.total()
            for k, slot in enumerate(part.g.slots):
                lines[:, k * rows : (k + 1) * rows] = totals[pl.ds(part.g.index(slot), 1), 0:rows]

        with jax.named_scope("sums_in"):
            inverse(image, row_tot, row_all)
            row_inv = row_all[...]
            row_inv_up = upright(row_inv)
            inverse(text, col_tot, col_all)
            col_inv = col_all[...]

        def scale(start, end):
            values = power[:, start:end] * (row_inv_up + col_inv[:, start:end])
            if start == 0:
                ids = [lax.broadcasted_iota(jnp.int32, values.shape, d) for d in (0, 1)]
                values = values - jnp.where((ids[0] == ids[1]) & (ids[0] < rows), 2.0, 0.0)
            pull[:, start:end] = values.astype(BF16)

        image.wait_sends(0)
        text.wait_sends(0)
        scaled = pull.shape[1]
        for s, first_slot, end_slot in BACK_ORDER:
            start, end = first_slot * rows, end_slot * rows
            part, own, out = ((image, image_own, image_out), (text, text_own, text_out))[s]
            with jax.named_scope(f"g{'it'[s]}{first_slot}"):
                if scaled > s * start:
                    scale(s * start, scaled)
                    scaled = s * start
                if s == 0:
                    grad = jnp.dot(pull[start:end, :], texts[...], preferred_element_type=F32)
                else:
                    grad = lax.dot_general(pull[:, start:end], images[...], TN, preferred_element_type=F32)
                own[start:end, :] = grad
                out[start:end, :] = grad.astype(BF16)
                part.send_ready(part.g.slots[first_slot:end_slot])
        image_loss[...] = -jnp.log(row_inv[:, 0:rows]) - matched
        text_loss[...] = -jnp.log(col_inv[:, 0:rows]) - matched
        for _, s, k in sorted((t, s, k) for s, part in enumerate((image, text)) for t, k in part.stops()):
            part = (image, text)[s]
            with jax.named_scope(f"pass_{'it'[s]}{k:02d}"):
                part.pass_on(k)
        image_grad[...] = image_own[0:rows, :]
        text_grad[...] = text_own[0:rows, :]
        with jax.named_scope("out"):
            for _, s, k in sorted((t, s, k) for s, part in enumerate((image, text)) for t, k in part.home_pools()):
                (image, text)[s].add_home(k, (image_grad, text_grad)[s])
        with jax.named_scope("wait_sends"):
            for part in (image, text):
                part.wait_sends(0)
                part.wait_sends(1)

    if len(PLANS) == 1:
        run(PLANS[0])
    else:
        for k, plan in enumerate(PLANS):
            pl.when(unit == k)(functools.partial(run, plan))


def place(*refs):
    sem = refs[-1]
    copies = [
        pltpu.make_async_copy(refs[i], refs[i + 4], sem.at[i]) for i in (2, 3, 0, 1)
    ]
    for copy in copies:
        copy.start()
    for copy in copies:
        copy.wait()


def solution(mesh):
    side = mesh.shape["lane"]

    def body(image_rows, text_rows):
        rows, width = image_rows.shape
        nz, npl = mesh.shape["block"] // side, side * side
        images_n, texts_n = nz * rows, npl * rows
        routes = [len(route[0]) for route in PLANS[0]]
        semaphores = (RECV_SEMS[0], RECV_SEMS[1])
        scratch = [
            pltpu.VMEM((rows, width), BF16),
            pltpu.VMEM((rows, width), BF16),
            pltpu.VMEM((images_n, width), BF16),
            pltpu.VMEM((texts_n, width), BF16),
            pltpu.VMEM((images_n, texts_n), F32),
            pltpu.VMEM((images_n, texts_n), BF16),
            pltpu.VMEM((nz, 128), F32),
            pltpu.VMEM((nz - 1, nz, 128), F32),
            pltpu.VMEM((npl, 128), F32),
            pltpu.VMEM((npl - 1, npl, 128), F32),
            pltpu.VMEM((nz, 128), F32),
            pltpu.VMEM((npl, 128), F32),
            pltpu.VMEM((1, images_n), F32),
            pltpu.VMEM((1, texts_n), F32),
            pltpu.VMEM((images_n, width), F32),
            pltpu.VMEM((texts_n, width), F32),
            pltpu.VMEM((images_n, width), BF16),
            pltpu.VMEM((texts_n, width), BF16),
            pltpu.VMEM((routes[0], rows // PIECES, width), BF16),
            pltpu.VMEM((routes[1], rows // PIECES, width), BF16),
        ]
        scratch.append(pltpu.SemaphoreType.REGULAR)
        for count in semaphores:
            scratch += [pltpu.SemaphoreType.DMA((n,)) for n in (2, count, 1)]
        results = pl.pallas_call(
            functools.partial(kernel, side),
            out_shape=(
                jax.ShapeDtypeStruct((1, rows), F32),
                jax.ShapeDtypeStruct((1, rows), F32),
                jax.ShapeDtypeStruct((rows, width), F32),
                jax.ShapeDtypeStruct((rows, width), F32),
            ),
            in_specs=[pl.BlockSpec(memory_space=pltpu.HBM)] * 2,
            out_specs=[pl.BlockSpec(memory_space=pltpu.VMEM)] * 4,
            scratch_shapes=scratch,
            compiler_params=pltpu.CompilerParams(
                collective_id=0, has_side_effects=True, vmem_limit_bytes=40 * 2**20
            ),
        )(*(pltpu.with_memory_space_constraint(x, pltpu.HBM) for x in (image_rows, text_rows)))
        image_loss, text_loss, image_grad, text_grad = pl.pallas_call(
            place,
            out_shape=tuple(jax.ShapeDtypeStruct(r.shape, r.dtype) for r in results),
            in_specs=[pl.BlockSpec(memory_space=pltpu.VMEM)] * 4,
            out_specs=[pl.BlockSpec(memory_space=pl.ANY)] * 4,
            scratch_shapes=[pltpu.SemaphoreType.DMA((4,))],
            compiler_params=pltpu.CompilerParams(vmem_limit_bytes=4 * rows * width * 8),
        )(*results)
        return (image_loss.reshape(rows), text_loss.reshape(rows), image_grad, text_grad)

    rows_spec = P(("unit", "block", "lane"), None)
    flat_spec = P(("unit", "block", "lane"))
    return jax.shard_map(
        body,
        mesh=mesh,
        in_specs=(rows_spec, rows_spec),
        out_specs=(flat_spec, flat_spec, rows_spec, rows_spec),
        check_vma=False,
    )
```

```python
import functools

import jax
import jax.numpy as jnp
from jax import lax
from jax.experimental import pallas as pl
from jax.experimental.pallas import tpu as pltpu
from jax.sharding import PartitionSpec as P

NT = (((1,), (1,)), ((), ()))
TN = (((0,), (0,)), ((), ()))
LOG2E = 1.4426950408889634
F32, BF16 = jnp.float32, jnp.bfloat16
PIECES = 2
RECV_SEMS = (10, 18)
BACK_ORDER = [(1, 12, 16), (0, 4, 8), (1, 8, 12), (0, 0, 4), (1, 4, 8), (1, 0, 4)]
IMAGE_GROUPS, TEXT_GROUPS = (4, 4), (4, 4, 8)

PLANS = [
    (
        (
            [
                ((4,), 1, (2,), 10.8), ((2,), 0, (1,), 6.9), ((3,), 0, (1,), 8.2), ((3,), 1, (1,), 9.5),
                ((6,), 0, (0,), 5.8), ((2,), 1, (0,), 5.8), ((7,), 1, (0,), 3.4), ((7,), 0, (0,), 4.1),
                ((6,), 1, (7,), 6.9), ((1,), 0, (0,), 3.4), ((5,), 0, (7,), 9.5), ((4,), 0, (6,), 10.8),
                ((1,), 1, (0,), 4.1), ((5,), 1, (7,), 8.2),
            ],
            [
                ((5,), 0, (6,), 4.3), ((1,), 0, (0,), 6.9), ((2,), 1, (0,), 8.8), ((6,), 0, (0,), 8.8),
                ((1,), 1, (0,), 7.5), ((3,), 1, (2,), 4.3), ((7,), 1, (0,), 6.9), ((5,), 1, (6,), 4.9),
                ((7,), 0, (0,), 7.5), ((6,), 1, (0,), 10.4), ((3,), 0, (2,), 4.9), ((4,), 0, (2,), 6.2),
                ((2,), 0, (0,), 10.4), ((4,), 1, (6,), 6.2),
            ],
        ),
        (
            [
                ((3, 2), 0, (3, 3), 10.8), ((2, 0), 1, (3, 0), 7.0), ((2, 3), 0, (1, 3), 10.3), ((1, 0), 0, (0, 0), 3.4),
                ((1, 1), 1, (0, 1), 7.0), ((0, 2), 0, (0, 3), 6.9), ((3, 0), 1, (0, 0), 3.4), ((0, 1), 1, (0, 0), 3.4),
                ((2, 2), 0, (1, 3), 10.9), ((0, 3), 0, (0, 0), 3.4), ((3, 1), 1, (0, 0), 5.7), ((1, 0), 1, (0, 0), 4.1),
                ((1, 3), 0, (0, 0), 5.7), ((3, 3), 1, (3, 0), 7.6), ((1, 1), 0, (0, 0), 6.4), ((3, 0), 0, (0, 0), 4.1),
                ((2, 2), 1, (3, 1), 10.1), ((1, 3), 1, (0, 3), 8.3), ((2, 1), 0, (3, 0), 8.8), ((2, 0), 0, (1, 0), 7.7),
                ((2, 1), 1, (3, 0), 7.7), ((0, 1), 0, (0, 0), 4.1), ((0, 2), 1, (0, 1), 7.6), ((3, 1), 0, (3, 0), 8.9),
                ((1, 2), 0, (1, 3), 10.2), ((3, 3), 0, (0, 0), 6.4), ((0, 3), 1, (0, 0), 4.1), ((1, 2), 1, (0, 3), 9.0),
                ((3, 2), 1, (3, 1), 10.2), ((2, 3), 1, (1, 0), 9.6),
            ],
            [
                ((3, 0), 0, (0, 0), 7.2), ((1, 0), 1, (0, 0), 7.8), ((2, 1), 1, (3, 1), 5.2), ((0, 3), 0, (0, 0), 10.7),
                ((2, 3), 1, (1, 3), 3.9), ((3, 1), 0, (0, 1), 5.9), ((2, 2), 1, (1, 3), 4.6), ((1, 1), 1, (0, 0), 8.6),
                ((3, 1), 1, (0, 0), 9.3), ((1, 2), 0, (1, 3), 4.6), ((2, 0), 0, (1, 0), 6.5), ((1, 3), 0, (0, 0), 9.9),
                ((0, 2), 1, (0, 1), 6.5), ((2, 3), 0, (3, 3), 3.9), ((3, 2), 0, (0, 1), 4.6), ((3, 0), 1, (0, 0), 10.0),
                ((1, 1), 0, (1, 0), 7.2), ((0, 3), 1, (0, 0), 5.9), ((2, 2), 0, (1, 3), 5.8), ((1, 2), 1, (1, 1), 4.6),
                ((3, 2), 1, (3, 1), 5.2), ((0, 1), 0, (0, 0), 9.4), ((3, 3), 1, (3, 0), 6.5), ((1, 0), 0, (0, 0), 10.7),
                ((2, 0), 1, (3, 0), 6.5), ((1, 3), 1, (0, 0), 9.3), ((0, 2), 0, (0, 3), 7.2), ((3, 3), 0, (0, 0), 8.4),
                ((2, 1), 0, (1, 0), 7.1), ((0, 1), 1, (0, 0), 10.0),
            ],
        ),
    ),
    (
        (
            [
                ((5,), 1, (6,), 7.1), ((6,), 1, (0,), 4.5), ((5,), 0, (7,), 5.8), ((7,), 0, (0,), 2.4),
                ((4,), 0, (5,), 8.3), ((6,), 0, (7,), 6.4), ((1,), 1, (0,), 2.4), ((2,), 0, (0,), 4.5),
                ((7,), 1, (0,), 3.1), ((3,), 1, (1,), 5.8), ((2,), 1, (1,), 6.4), ((3,), 0, (2,), 7.1),
                ((1,), 0, (0,), 3.1), ((4,), 1, (3,), 8.3),
            ],
            [
                ((7,), 0, (0,), 4.6), ((1,), 1, (0,), 4.6), ((2,), 0, (0,), 9.0), ((3,), 0, (2,), 5.9),
                ((4,), 0, (3,), 3.3), ((3,), 1, (2,), 3.9), ((1,), 0, (0,), 5.2), ((5,), 1, (6,), 5.9),
                ((2,), 1, (0,), 7.2), ((6,), 1, (0,), 9.0), ((4,), 1, (5,), 3.3), ((6,), 0, (0,), 7.2),
                ((5,), 0, (6,), 3.9), ((7,), 1, (0,), 5.2),
            ],
        ),
        (
            [
                ((1, 2), 1, (1, 1), 8.0), ((1, 1), 1, (0, 1), 5.1), ((2, 2), 1, (2, 3), 8.6), ((2, 3), 1, (1, 0), 6.1),
                ((1, 0), 0, (0, 0), 2.4), ((3, 0), 1, (0, 0), 2.4), ((3, 1), 1, (0, 0), 4.4), ((3, 0), 0, (0, 0), 3.1),
                ((0, 3), 0, (0, 0), 2.4), ((1, 1), 0, (1, 0), 4.9), ((0, 2), 1, (0, 3), 6.2), ((1, 2), 0, (1, 1), 7.4),
                ((3, 3), 0, (0, 3), 5.1), ((0, 1), 1, (0, 0), 2.4), ((3, 3), 1, (3, 0), 4.9), ((2, 1), 1, (3, 1), 7.0),
                ((3, 2), 1, (3, 3), 7.5), ((2, 0), 0, (3, 0), 6.4), ((2, 1), 0, (1, 1), 8.1), ((1, 3), 0, (0, 0), 4.4),
                ((2, 3), 0, (3, 3), 7.7), ((3, 1), 0, (3, 0), 5.6), ((1, 3), 1, (0, 3), 6.8), ((2, 2), 0, (1, 3), 7.5),
                ((2, 0), 1, (3, 0), 5.7), ((0, 3), 1, (0, 0), 3.1), ((1, 0), 1, (0, 0), 3.1), ((0, 1), 0, (0, 0), 3.1),
                ((0, 2), 0, (0, 1), 6.2), ((3, 2), 0, (0, 2), 8.7),
            ],
            [
                ((0, 3), 0, (0, 0), 6.8), ((2, 2), 1, (1, 2), 2.9), ((0, 2), 0, (0, 1), 4.9), ((1, 1), 0, (0, 1), 4.9),
                ((1, 1), 1, (0, 1), 5.5), ((1, 3), 1, (1, 0), 3.6), ((2, 0), 1, (3, 0), 4.9), ((2, 0), 0, (1, 0), 3.6),
                ((1, 3), 0, (0, 0), 8.1), ((3, 2), 1, (3, 1), 2.9), ((3, 1), 0, (0, 0), 7.3), ((3, 3), 0, (3, 0), 5.5),
                ((2, 1), 0, (3, 1), 2.9), ((0, 1), 0, (0, 0), 7.4), ((0, 3), 1, (0, 0), 8.1), ((0, 1), 1, (0, 0), 8.7),
                ((0, 2), 1, (0, 3), 4.2), ((2, 3), 0, (1, 3), 4.2), ((3, 1), 1, (0, 1), 6.2), ((1, 0), 0, (0, 0), 6.8),
                ((2, 1), 1, (3, 1), 3.6), ((2, 2), 0, (3, 1), 4.2), ((1, 0), 1, (0, 0), 7.5), ((1, 2), 0, (1, 3), 2.9),
                ((1, 2), 1, (0, 1), 6.2), ((3, 2), 0, (3, 1), 4.2), ((3, 3), 1, (3, 0), 6.2), ((2, 3), 1, (3, 0), 5.5),
                ((3, 0), 0, (0, 0), 8.0), ((3, 0), 1, (0, 0), 8.7),
            ],
        ),
    ),
]


def rectangles(cells):
    found = []
    for h in sorted({h for h, _ in cells}):
        runs = []
        for g in sorted(g for k, g in cells if k == h):
            if runs and runs[-1][-1] == g - 1:
                runs[-1].append(g)
            else:
                runs.append([g])
        for run in runs:
            match = [hs for hs, gs in found if gs == run and hs[-1] == h - 1]
            if match:
                match[0].append(h)
            else:
                found.append(([h], run))
    return found


class Group:
    def __init__(self, route, sizes, here, device):
        self.sizes, self.here, self.device_of = sizes, here, device
        self.home = (0,) * len(sizes)
        when = {self.home: 0.0}
        for o, _, _, t in route:
            when[self.neg(o)] = max(t, when.get(self.neg(o), 0.0))
        self.slots = sorted(when, key=when.get)

    def sub(self, a, b):
        return tuple((i - j) % n for i, j, n in zip(a, b, self.sizes))

    def neg(self, a):
        return tuple(-i % n for i, n in zip(a, self.sizes))

    def at(self, a):
        return [lax.rem(h + i, n) if i else h for h, i, n in zip(self.here, a, self.sizes)]

    def device(self, a):
        return self.device_of(*self.at(a))

    def index(self, a):
        index = 0
        for i, n in zip(self.at(a), self.sizes):
            index = index * n + i
        return index


def unit_rows(values):
    wide = values.astype(F32)
    scale = lax.rsqrt(jnp.sum(wide * wide, axis=-1, keepdims=True) + 1e-06)
    return (wide * scale).astype(BF16)


def upright(row):
    return jnp.transpose(jnp.broadcast_to(row, (8, row.shape[1])))[:, :1]


class Side:
    def __init__(self, group, group_of, routes, rows, data, sums, mine, own, out, inbox, sems):
        self.g, self.rows, self.data, self.sums, self.mine = group, rows, data, sums, mine
        self.out_route, self.back_route = routes
        self.own, self.out, self.inbox = own, out, inbox
        self.send, self.recv, self.sum_recv = sems
        self.pos = {slot: k for k, slot in enumerate(group.slots)}
        self.home = group.home
        self.landed = set()
        g = group

        def remote(send, src, dst, recv, offset):
            return pltpu.make_async_remote_copy(
                src_ref=src, dst_ref=dst, send_sem=self.send.at[send], recv_sem=recv, device_id=g.device(offset)
            )

        self.out_pools, self.back_pools = self.pools(group_of)
        assert max(len(self.out_pools), len(self.back_pools)) <= self.recv.shape[0]
        out_pool, back_pool = ({k: n for n, ks in enumerate(pools) for k in ks} for pools in (self.out_pools, self.back_pools))
        self.gather = [
            remote(
                0, data.at[self.piece(g.neg(r), p)], data.at[self.piece(g.neg(o), p)],
                self.recv.at[out_pool[k]], g.sub(o, r),
            )
            for k, (o, p, r, _) in enumerate(self.out_route)
        ]
        self.exchange = [
            remote(1, mine, sums.at[k], self.sum_recv.at[0], o) for k, o in enumerate(reversed(g.slots[1:]))
        ]
        self.reduce = [
            remote(0, out.at[self.piece(g.neg(o), p)], inbox.at[k], self.recv.at[back_pool[k]], g.sub(r, o))
            for k, (o, p, r, _) in enumerate(self.back_route)
        ]

    def pools(self, group_of):
        out, back = {}, {}
        for k, (o, p, _, _) in enumerate(self.out_route):
            out.setdefault(("at", k) if self.onward(o, p) else ("of", group_of[self.pos[self.g.neg(o)]]), []).append(k)
        for k, (_, p, r, _) in enumerate(self.back_route):
            if r != self.home:
                back.setdefault((r, p), []).append(k)
        home = [k for _, k in sorted(self.home_parts())]
        while home:
            count = min(4, max(1, len(home) // 2))
            back[home[0]], home = home[:count], home[count:]
        return list(out.values()), list(back.values())

    def wait_pool(self, pools, n):
        amount = self.inbox.at[pl.ds(0, len(pools[n]))]
        pltpu.make_async_copy(amount, amount, self.recv.at[n]).wait()

    def hops(self, offset):
        return sum(min(i, n - i) for i, n in zip(offset, self.g.sizes))

    def next_to(self):
        return [o for o in self.g.slots if self.hops(o) == 1]

    def piece(self, slot, p):
        size = self.rows // PIECES
        return pl.ds(self.pos[slot] * self.rows + p * size, size)

    def onward(self, o, p):
        return [k for k, (_, q, r, _) in enumerate(self.out_route) if r == o and q == p]

    def inward(self, o, p):
        parts = [(t, k) for k, (_, q, r, t) in enumerate(self.back_route) if r == o and q == p]
        return [k for _, k in sorted(parts)]

    def start_gather(self, hops):
        for k, (o, _, r, _) in enumerate(self.out_route):
            if r == self.home and self.hops(o) == hops:
                self.gather[k].start()

    def arrive(self, k):
        o, p, _, _ = self.out_route[k]
        pool = [n for n, ks in enumerate(self.out_pools) if k in ks][0]
        self.landed.add(k)
        if not self.landed.issuperset(self.out_pools[pool]):
            return
        self.wait_pool(self.out_pools, pool)
        for j in self.onward(o, p):
            assert self.hops(self.g.sub(self.out_route[j][0], o)) <= 2
            self.gather[j].start()

    def keep_sum(self, position, row):
        slot = self.g.slots[position]
        self.mine[pl.ds(self.g.index(slot), 1), 0 : self.rows] = row

    def start_sums(self):
        for copy in self.exchange:
            copy.start()

    def total(self):
        pltpu.make_async_copy(self.sums, self.sums, self.sum_recv.at[0]).wait()
        total = self.mine[...]
        for k in range(len(self.exchange)):
            total = total + self.sums[k]
        return total

    def send_ready(self, slots):
        for k, (o, p, _, _) in enumerate(self.back_route):
            if self.g.neg(o) in slots and not self.inward(o, p):
                self.reduce[k].start()

    def stops(self):
        parts = [(self.inward(o, p), k) for k, (o, p, _, _) in enumerate(self.back_route)]
        return [(self.back_route[inward[-1]][3], k) for inward, k in parts if inward]

    def pass_on(self, k):
        o, p, _, _ = self.back_route[k]
        where = self.piece(self.g.neg(o), p)
        total = self.own[where, :]
        parts = self.inward(o, p)
        self.wait_pool(self.back_pools, [n for n, ks in enumerate(self.back_pools) if parts[0] in ks][0])
        for j in parts:
            total = total + self.inbox[j].astype(F32)
        self.out[where, :] = total.astype(BF16)
        self.reduce[k].start()

    def home_parts(self):
        return [(t, k) for k, (_, _, r, t) in enumerate(self.back_route) if r == self.home]

    def home_pools(self):
        when = dict((k, t) for t, k in self.home_parts())
        return [(max(when[k] for k in ks), n) for n, ks in enumerate(self.back_pools) if ks[0] in when]

    def add_home(self, n, grad):
        size = self.rows // PIECES
        self.wait_pool(self.back_pools, n)
        for p in range(PIECES):
            parts = [k for k in self.back_pools[n] if self.back_route[k][1] == p]
            if parts:
                here = slice(p * size, (p + 1) * size)
                grad[here, :] = sum((self.inbox[k].astype(F32) for k in parts), grad[here, :])

    def wait_sends(self, n):
        amount = (self.inbox, self.sums)[n]
        pltpu.make_async_copy(amount, amount, self.send.at[n]).wait()


def kernel(
    side,
    image_hbm, text_hbm,
    image_loss, text_loss, image_grad, text_grad,
    image_raw, text_raw, images, texts, power, pull,
    row_mine, row_in, col_mine, col_in, row_tot, col_tot, row_all, col_all,
    image_own, text_own, image_out, text_out, image_box, text_box,
    around, *sems,
):
    lane, block, unit = lax.axis_index("lane"), lax.axis_index("block"), lax.axis_index("unit")
    z, y = block // side, lax.rem(block, side)
    rows = image_raw.shape[0]
    image_count = row_mine.shape[0]
    sizes = (IMAGE_GROUPS, TEXT_GROUPS)
    first = [[sum(s[:g]) for g in range(len(s) + 1)] for s in sizes]
    group_of = [[g for g, n in enumerate(s) for _ in range(n)] for s in sizes]

    loads = [
        pltpu.make_async_copy(image_hbm, image_raw, sems[0].at[0]),
        pltpu.make_async_copy(text_hbm, text_raw, sems[3].at[0]),
    ]
    for load in loads:
        load.start()
    barrier = pltpu.get_barrier_semaphore()

    def sides(plan):
        line = Group(plan[0][0], (image_count,), (z,), lambda k: {"block": k * side + y})
        plane = Group(plan[1][0], (side, side), (y, lane), lambda k, j: {"block": z * side + k, "lane": j})
        return (
            Side(line, group_of[0], plan[0], rows, images, row_in, row_mine, image_own, image_out, image_box, sems[:3]),
            Side(plane, group_of[1], plan[1], rows, texts, col_in, col_mine, text_own, text_out, text_box, sems[3:]),
        )

    def some(s, gs):
        start, end = first[s][gs[0]] * rows, first[s][gs[-1] + 1] * rows
        return pl.ds(start, end - start)

    def run(plan):
        image, text = sides(plan)
        for part in (image, text):
            for o in part.next_to():
                pl.semaphore_signal(barrier, inc=1, device_id=part.g.device(o))
        with jax.named_scope("load"):
            loads[1].wait()
            texts[0:rows, :] = unit_rows(text_raw[...])
            loads[0].wait()
            images[0:rows, :] = unit_rows(image_raw[...])
        with jax.named_scope("barrier"):
            pl.semaphore_wait(barrier, len(image.next_to()) + len(text.next_to()))
        for part in (image, text):
            for o in part.next_to():
                pl.semaphore_signal(around, inc=1, device_id=part.g.device(o))
        text.start_gather(1)
        image.start_gather(1)

        with jax.named_scope("around"):
            pl.semaphore_wait(around, len(image.next_to()) + len(text.next_to()))
        text.start_gather(2)
        image.start_gather(2)

        pair = 12.0 * lax.dot_general(images[0:rows, :], texts[0:rows, :], NT, preferred_element_type=F32)
        eye = lax.broadcasted_iota(jnp.int32, (rows, rows), 0) == lax.broadcasted_iota(jnp.int32, (rows, rows), 1)
        matched = jnp.sum(jnp.where(eye, pair, 0.0), axis=0, keepdims=True)

        row_sums, col_sums = [0.0] * len(IMAGE_GROUPS), [0.0] * len(TEXT_GROUPS)

        def powers(hs, gs):
            here, there = some(0, hs), some(1, gs)
            logit = lax.dot_general(images[here, :], texts[there, :], NT, preferred_element_type=F32)
            p = jnp.exp2((12.0 * LOG2E) * logit)
            power[here, there] = p
            lanes = sum(p[:, k : k + 128] for k in range(0, p.shape[1], 128))
            for s, groups, sums in ((0, hs, row_sums), (1, gs, col_sums)):
                start = 0
                for g in groups:
                    end = start + sizes[s][g] * rows
                    sums[g] += jnp.sum(p[:, start:end], axis=0, keepdims=True) if s else lanes[start:end]
                    start = end

        def keep_sums(s, g):
            part, row = (image, text)[s], (row_sums, col_sums)[s][g]
            row = row if s else jnp.sum(jnp.transpose(row), axis=0, keepdims=True)
            for k in range(sizes[s][g]):
                part.keep_sum(first[s][g] + k, row[:, k * rows : (k + 1) * rows])

        waits = sorted(
            (t, s, k) for s, part in enumerate((image, text)) for k, (_, _, _, t) in enumerate(part.out_route)
        )
        missing = {(s, g): set() for s in (0, 1) for g in range(len(sizes[s]))}
        for s, part in enumerate((image, text)):
            for k, (o, _, _, _) in enumerate(part.out_route):
                missing[(s, group_of[s][part.pos[part.g.neg(o)]])].add(k)
        todo = {(h, g) for h in range(len(IMAGE_GROUPS)) for g in range(len(TEXT_GROUPS))}
        for _, s, k in waits:
            part = (image, text)[s]
            with jax.named_scope(f"arrive_{'it'[s]}{k:02d}"):
                part.arrive(k)
            missing[(s, group_of[s][part.pos[part.g.neg(part.out_route[k][0])]])].discard(k)
            ready = {(h, g) for h, g in todo if not missing[(0, h)] and not missing[(1, g)]}
            todo -= ready
            for hs, gs in rectangles(ready):
                with jax.named_scope(f"pow{hs[0]}{gs[0]}"):
                    powers(hs, gs)
            for g in sorted({g for _, g in ready} - {g for _, g in todo}):
                keep_sums(1, g)

        with jax.named_scope("sums_out"):
            text.start_sums()
            for h in range(len(IMAGE_GROUPS)):
                keep_sums(0, h)
            image.start_sums()

        def inverse(part, totals, lines):
            totals[...] = 1.0 / part.total()
            for k, slot in enumerate(part.g.slots):
                lines[:, k * rows : (k + 1) * rows] = totals[pl.ds(part.g.index(slot), 1), 0:rows]

        with jax.named_scope("sums_in"):
            inverse(image, row_tot, row_all)
            row_inv = row_all[...]
            row_inv_up = upright(row_inv)
            inverse(text, col_tot, col_all)
            col_inv = col_all[...]

        def scale(start, end):
            values = power[:, start:end] * (row_inv_up + col_inv[:, start:end])
            if start == 0:
                ids = [lax.broadcasted_iota(jnp.int32, values.shape, d) for d in (0, 1)]
                values = values - jnp.where((ids[0] == ids[1]) & (ids[0] < rows), 2.0, 0.0)
            pull[:, start:end] = values.astype(BF16)

        image.wait_sends(0)
        text.wait_sends(0)
        scaled = pull.shape[1]
        for s, first_slot, end_slot in BACK_ORDER:
            start, end = first_slot * rows, end_slot * rows
            part, own, out = ((image, image_own, image_out), (text, text_own, text_out))[s]
            with jax.named_scope(f"g{'it'[s]}{first_slot}"):
                if scaled > s * start:
                    scale(s * start, scaled)
                    scaled = s * start
                if s == 0:
                    grad = jnp.dot(pull[start:end, :], texts[...], preferred_element_type=F32)
                else:
                    grad = lax.dot_general(pull[:, start:end], images[...], TN, preferred_element_type=F32)
                own[start:end, :] = grad
                out[start:end, :] = grad.astype(BF16)
                part.send_ready(part.g.slots[first_slot:end_slot])
        image_loss[...] = -jnp.log(row_inv[:, 0:rows]) - matched
        text_loss[...] = -jnp.log(col_inv[:, 0:rows]) - matched
        for _, s, k in sorted((t, s, k) for s, part in enumerate((image, text)) for t, k in part.stops()):
            part = (image, text)[s]
            with jax.named_scope(f"pass_{'it'[s]}{k:02d}"):
                part.pass_on(k)
        image_grad[...] = image_own[0:rows, :]
        text_grad[...] = text_own[0:rows, :]
        with jax.named_scope("out"):
            for _, s, k in sorted((t, s, k) for s, part in enumerate((image, text)) for t, k in part.home_pools()):
                (image, text)[s].add_home(k, (image_grad, text_grad)[s])
        with jax.named_scope("wait_sends"):
            for part in (image, text):
                part.wait_sends(0)
                part.wait_sends(1)

    if len(PLANS) == 1:
        run(PLANS[0])
    else:
        for k, plan in enumerate(PLANS):
            pl.when(unit == k)(functools.partial(run, plan))


def place(*refs):
    sem = refs[-1]
    copies = [
        pltpu.make_async_copy(refs[i], refs[i + 4], sem.at[i]) for i in (2, 3, 0, 1)
    ]
    for copy in copies:
        copy.start()
    for copy in copies:
        copy.wait()


def solution(mesh):
    side = mesh.shape["lane"]

    def body(image_rows, text_rows):
        rows, width = image_rows.shape
        nz, npl = mesh.shape["block"] // side, side * side
        images_n, texts_n = nz * rows, npl * rows
        routes = [len(route[0]) for route in PLANS[0]]
        semaphores = (RECV_SEMS[0], RECV_SEMS[1])
        scratch = [
            pltpu.VMEM((rows, width), BF16),
            pltpu.VMEM((rows, width), BF16),
            pltpu.VMEM((images_n, width), BF16),
            pltpu.VMEM((texts_n, width), BF16),
            pltpu.VMEM((images_n, texts_n), F32),
            pltpu.VMEM((images_n, texts_n), BF16),
            pltpu.VMEM((nz, 128), F32),
            pltpu.VMEM((nz - 1, nz, 128), F32),
            pltpu.VMEM((npl, 128), F32),
            pltpu.VMEM((npl - 1, npl, 128), F32),
            pltpu.VMEM((nz, 128), F32),
            pltpu.VMEM((npl, 128), F32),
            pltpu.VMEM((1, images_n), F32),
            pltpu.VMEM((1, texts_n), F32),
            pltpu.VMEM((images_n, width), F32),
            pltpu.VMEM((texts_n, width), F32),
            pltpu.VMEM((images_n, width), BF16),
            pltpu.VMEM((texts_n, width), BF16),
            pltpu.VMEM((routes[0], rows // PIECES, width), BF16),
            pltpu.VMEM((routes[1], rows // PIECES, width), BF16),
        ]
        scratch.append(pltpu.SemaphoreType.REGULAR)
        for count in semaphores:
            scratch += [pltpu.SemaphoreType.DMA((n,)) for n in (2, count, 1)]
        results = pl.pallas_call(
            functools.partial(kernel, side),
            out_shape=(
                jax.ShapeDtypeStruct((1, rows), F32),
                jax.ShapeDtypeStruct((1, rows), F32),
                jax.ShapeDtypeStruct((rows, width), F32),
                jax.ShapeDtypeStruct((rows, width), F32),
            ),
            in_specs=[pl.BlockSpec(memory_space=pltpu.HBM)] * 2,
            out_specs=[pl.BlockSpec(memory_space=pltpu.VMEM)] * 4,
            scratch_shapes=scratch,
            compiler_params=pltpu.CompilerParams(
                collective_id=0, has_side_effects=True, vmem_limit_bytes=40 * 2**20
            ),
        )(*(pltpu.with_memory_space_constraint(x, pltpu.HBM) for x in (image_rows, text_rows)))
        image_loss, text_loss, image_grad, text_grad = pl.pallas_call(
            place,
            out_shape=tuple(jax.ShapeDtypeStruct(r.shape, r.dtype) for r in results),
            in_specs=[pl.BlockSpec(memory_space=pltpu.VMEM)] * 4,
            out_specs=[pl.BlockSpec(memory_space=pl.ANY)] * 4,
            scratch_shapes=[pltpu.SemaphoreType.DMA((4,))],
            compiler_params=pltpu.CompilerParams(vmem_limit_bytes=4 * rows * width * 8),
        )(*results)
        return (image_loss.reshape(rows), text_loss.reshape(rows), image_grad, text_grad)

    rows_spec = P(("unit", "block", "lane"), None)
    flat_spec = P(("unit", "block", "lane"))
    return jax.shard_map(
        body,
        mesh=mesh,
        in_specs=(rows_spec, rows_spec),
        out_specs=(flat_spec, flat_spec, rows_spec, rows_spec),
        check_vma=False,
    )
```

```python
import functools

import jax
import jax.numpy as jnp
from jax import lax
from jax.experimental import pallas as pl
from jax.experimental.pallas import tpu as pltpu
from jax.sharding import PartitionSpec as P

NT = (((1,), (1,)), ((), ()))
TN = (((0,), (0,)), ((), ()))
LOG2E = 1.4426950408889634
F32, BF16 = jnp.float32, jnp.bfloat16
PIECES = 2
RECV_SEMS = (10, 18)
BACK_ORDER = [(1, 12, 16), (0, 4, 8), (1, 8, 12), (0, 0, 4), (1, 4, 8), (1, 0, 4)]
IMAGE_GROUPS, TEXT_GROUPS = (4, 4), (4, 4, 8)

PLANS = [
    (
        (
            [
                ((4,), 1, (2,), 10.8), ((2,), 0, (1,), 6.9), ((3,), 0, (1,), 8.2), ((3,), 1, (1,), 9.5),
                ((6,), 0, (0,), 5.8), ((2,), 1, (0,), 5.8), ((7,), 1, (0,), 3.4), ((7,), 0, (0,), 4.1),
                ((6,), 1, (7,), 6.9), ((1,), 0, (0,), 3.4), ((5,), 0, (7,), 9.5), ((4,), 0, (6,), 10.8),
                ((1,), 1, (0,), 4.1), ((5,), 1, (7,), 8.2),
            ],
            [
                ((5,), 0, (6,), 4.3), ((1,), 0, (0,), 6.9), ((2,), 1, (0,), 8.8), ((6,), 0, (0,), 8.8),
                ((1,), 1, (0,), 7.5), ((3,), 1, (2,), 4.3), ((7,), 1, (0,), 6.9), ((5,), 1, (6,), 4.9),
                ((7,), 0, (0,), 7.5), ((6,), 1, (0,), 10.4), ((3,), 0, (2,), 4.9), ((4,), 0, (2,), 6.2),
                ((2,), 0, (0,), 10.4), ((4,), 1, (6,), 6.2),
            ],
        ),
        (
            [
                ((3, 2), 0, (3, 3), 10.8), ((2, 0), 1, (3, 0), 7.0), ((2, 3), 0, (1, 3), 10.3), ((1, 0), 0, (0, 0), 3.4),
                ((1, 1), 1, (0, 1), 7.0), ((0, 2), 0, (0, 3), 6.9), ((3, 0), 1, (0, 0), 3.4), ((0, 1), 1, (0, 0), 3.4),
                ((2, 2), 0, (1, 3), 10.9), ((0, 3), 0, (0, 0), 3.4), ((3, 1), 1, (0, 0), 5.7), ((1, 0), 1, (0, 0), 4.1),
                ((1, 3), 0, (0, 0), 5.7), ((3, 3), 1, (3, 0), 7.6), ((1, 1), 0, (0, 0), 6.4), ((3, 0), 0, (0, 0), 4.1),
                ((2, 2), 1, (3, 1), 10.1), ((1, 3), 1, (0, 3), 8.3), ((2, 1), 0, (3, 0), 8.8), ((2, 0), 0, (1, 0), 7.7),
                ((2, 1), 1, (3, 0), 7.7), ((0, 1), 0, (0, 0), 4.1), ((0, 2), 1, (0, 1), 7.6), ((3, 1), 0, (3, 0), 8.9),
                ((1, 2), 0, (1, 3), 10.2), ((3, 3), 0, (0, 0), 6.4), ((0, 3), 1, (0, 0), 4.1), ((1, 2), 1, (0, 3), 9.0),
                ((3, 2), 1, (3, 1), 10.2), ((2, 3), 1, (1, 0), 9.6),
            ],
            [
                ((3, 0), 0, (0, 0), 7.2), ((1, 0), 1, (0, 0), 7.8), ((2, 1), 1, (3, 1), 5.2), ((0, 3), 0, (0, 0), 10.7),
                ((2, 3), 1, (1, 3), 3.9), ((3, 1), 0, (0, 1), 5.9), ((2, 2), 1, (1, 3), 4.6), ((1, 1), 1, (0, 0), 8.6),
                ((3, 1), 1, (0, 0), 9.3), ((1, 2), 0, (1, 3), 4.6), ((2, 0), 0, (1, 0), 6.5), ((1, 3), 0, (0, 0), 9.9),
                ((0, 2), 1, (0, 1), 6.5), ((2, 3), 0, (3, 3), 3.9), ((3, 2), 0, (0, 1), 4.6), ((3, 0), 1, (0, 0), 10.0),
                ((1, 1), 0, (1, 0), 7.2), ((0, 3), 1, (0, 0), 5.9), ((2, 2), 0, (1, 3), 5.8), ((1, 2), 1, (1, 1), 4.6),
                ((3, 2), 1, (3, 1), 5.2), ((0, 1), 0, (0, 0), 9.4), ((3, 3), 1, (3, 0), 6.5), ((1, 0), 0, (0, 0), 10.7),
                ((2, 0), 1, (3, 0), 6.5), ((1, 3), 1, (0, 0), 9.3), ((0, 2), 0, (0, 3), 7.2), ((3, 3), 0, (0, 0), 8.4),
                ((2, 1), 0, (1, 0), 7.1), ((0, 1), 1, (0, 0), 10.0),
            ],
        ),
    ),
    (
        (
            [
                ((5,), 1, (6,), 7.1), ((6,), 1, (0,), 4.5), ((5,), 0, (7,), 5.8), ((7,), 0, (0,), 2.4),
                ((4,), 0, (5,), 8.3), ((6,), 0, (7,), 6.4), ((1,), 1, (0,), 2.4), ((2,), 0, (0,), 4.5),
                ((7,), 1, (0,), 3.1), ((3,), 1, (1,), 5.8), ((2,), 1, (1,), 6.4), ((3,), 0, (2,), 7.1),
                ((1,), 0, (0,), 3.1), ((4,), 1, (3,), 8.3),
            ],
            [
                ((7,), 0, (0,), 4.6), ((1,), 1, (0,), 4.6), ((2,), 0, (0,), 9.0), ((3,), 0, (2,), 5.9),
                ((4,), 0, (3,), 3.3), ((3,), 1, (2,), 3.9), ((1,), 0, (0,), 5.2), ((5,), 1, (6,), 5.9),
                ((2,), 1, (0,), 7.2), ((6,), 1, (0,), 9.0), ((4,), 1, (5,), 3.3), ((6,), 0, (0,), 7.2),
                ((5,), 0, (6,), 3.9), ((7,), 1, (0,), 5.2),
            ],
        ),
        (
            [
                ((1, 2), 1, (1, 1), 8.0), ((1, 1), 1, (0, 1), 5.1), ((2, 2), 1, (2, 3), 8.6), ((2, 3), 1, (1, 0), 6.1),
                ((1, 0), 0, (0, 0), 2.4), ((3, 0), 1, (0, 0), 2.4), ((3, 1), 1, (0, 0), 4.4), ((3, 0), 0, (0, 0), 3.1),
                ((0, 3), 0, (0, 0), 2.4), ((1, 1), 0, (1, 0), 4.9), ((0, 2), 1, (0, 3), 6.2), ((1, 2), 0, (1, 1), 7.4),
                ((3, 3), 0, (0, 3), 5.1), ((0, 1), 1, (0, 0), 2.4), ((3, 3), 1, (3, 0), 4.9), ((2, 1), 1, (3, 1), 7.0),
                ((3, 2), 1, (3, 3), 7.5), ((2, 0), 0, (3, 0), 6.4), ((2, 1), 0, (1, 1), 8.1), ((1, 3), 0, (0, 0), 4.4),
                ((2, 3), 0, (3, 3), 7.7), ((3, 1), 0, (3, 0), 5.6), ((1, 3), 1, (0, 3), 6.8), ((2, 2), 0, (1, 3), 7.5),
                ((2, 0), 1, (3, 0), 5.7), ((0, 3), 1, (0, 0), 3.1), ((1, 0), 1, (0, 0), 3.1), ((0, 1), 0, (0, 0), 3.1),
                ((0, 2), 0, (0, 1), 6.2), ((3, 2), 0, (0, 2), 8.7),
            ],
            [
                ((0, 3), 0, (0, 0), 6.8), ((2, 2), 1, (1, 2), 2.9), ((0, 2), 0, (0, 1), 4.9), ((1, 1), 0, (0, 1), 4.9),
                ((1, 1), 1, (0, 1), 5.5), ((1, 3), 1, (1, 0), 3.6), ((2, 0), 1, (3, 0), 4.9), ((2, 0), 0, (1, 0), 3.6),
                ((1, 3), 0, (0, 0), 8.1), ((3, 2), 1, (3, 1), 2.9), ((3, 1), 0, (0, 0), 7.3), ((3, 3), 0, (3, 0), 5.5),
                ((2, 1), 0, (3, 1), 2.9), ((0, 1), 0, (0, 0), 7.4), ((0, 3), 1, (0, 0), 8.1), ((0, 1), 1, (0, 0), 8.7),
                ((0, 2), 1, (0, 3), 4.2), ((2, 3), 0, (1, 3), 4.2), ((3, 1), 1, (0, 1), 6.2), ((1, 0), 0, (0, 0), 6.8),
                ((2, 1), 1, (3, 1), 3.6), ((2, 2), 0, (3, 1), 4.2), ((1, 0), 1, (0, 0), 7.5), ((1, 2), 0, (1, 3), 2.9),
                ((1, 2), 1, (0, 1), 6.2), ((3, 2), 0, (3, 1), 4.2), ((3, 3), 1, (3, 0), 6.2), ((2, 3), 1, (3, 0), 5.5),
                ((3, 0), 0, (0, 0), 8.0), ((3, 0), 1, (0, 0), 8.7),
            ],
        ),
    ),
]


def rectangles(cells):
    found = []
    for h in sorted({h for h, _ in cells}):
        runs = []
        for g in sorted(g for k, g in cells if k == h):
            if runs and runs[-1][-1] == g - 1:
                runs[-1].append(g)
            else:
                runs.append([g])
        for run in runs:
            match = [hs for hs, gs in found if gs == run and hs[-1] == h - 1]
            if match:
                match[0].append(h)
            else:
                found.append(([h], run))
    return found


class Group:
    def __init__(self, route, sizes, here, device):
        self.sizes, self.here, self.device_of = sizes, here, device
        self.home = (0,) * len(sizes)
        when = {self.home: 0.0}
        for o, _, _, t in route:
            when[self.neg(o)] = max(t, when.get(self.neg(o), 0.0))
        self.slots = sorted(when, key=when.get)

    def sub(self, a, b):
        return tuple((i - j) % n for i, j, n in zip(a, b, self.sizes))

    def neg(self, a):
        return tuple(-i % n for i, n in zip(a, self.sizes))

    def at(self, a):
        return [lax.rem(h + i, n) if i else h for h, i, n in zip(self.here, a, self.sizes)]

    def device(self, a):
        return self.device_of(*self.at(a))

    def index(self, a):
        index = 0
        for i, n in zip(self.at(a), self.sizes):
            index = index * n + i
        return index


def unit_rows(values):
    wide = values.astype(F32)
    scale = lax.rsqrt(jnp.sum(wide * wide, axis=-1, keepdims=True) + 1e-06)
    return (wide * scale).astype(BF16)


def upright(row):
    return jnp.transpose(jnp.broadcast_to(row, (8, row.shape[1])))[:, :1]


class Side:
    def __init__(self, group, group_of, routes, rows, data, sums, mine, own, out, inbox, sems):
        self.g, self.rows, self.data, self.sums, self.mine = group, rows, data, sums, mine
        self.out_route, self.back_route = routes
        self.own, self.out, self.inbox = own, out, inbox
        self.send, self.recv, self.sum_recv = sems
        self.pos = {slot: k for k, slot in enumerate(group.slots)}
        self.home = group.home
        self.landed = set()
        g = group

        def remote(send, src, dst, recv, offset):
            return pltpu.make_async_remote_copy(
                src_ref=src, dst_ref=dst, send_sem=self.send.at[send], recv_sem=recv, device_id=g.device(offset)
            )

        self.out_pools, self.back_pools = self.pools(group_of)
        assert max(len(self.out_pools), len(self.back_pools)) <= self.recv.shape[0]
        out_pool, back_pool = ({k: n for n, ks in enumerate(pools) for k in ks} for pools in (self.out_pools, self.back_pools))
        self.gather = [
            remote(
                0, data.at[self.piece(g.neg(r), p)], data.at[self.piece(g.neg(o), p)],
                self.recv.at[out_pool[k]], g.sub(o, r),
            )
            for k, (o, p, r, _) in enumerate(self.out_route)
        ]
        self.exchange = [
            remote(1, mine, sums.at[k], self.sum_recv.at[0], o) for k, o in enumerate(reversed(g.slots[1:]))
        ]
        self.reduce = [
            remote(0, out.at[self.piece(g.neg(o), p)], inbox.at[k], self.recv.at[back_pool[k]], g.sub(r, o))
            for k, (o, p, r, _) in enumerate(self.back_route)
        ]

    def pools(self, group_of):
        out, back = {}, {}
        for k, (o, p, _, _) in enumerate(self.out_route):
            out.setdefault(("at", k) if self.onward(o, p) else ("of", group_of[self.pos[self.g.neg(o)]]), []).append(k)
        for k, (_, p, r, _) in enumerate(self.back_route):
            if r != self.home:
                back.setdefault((r, p), []).append(k)
        home = [k for _, k in sorted(self.home_parts())]
        while home:
            count = min(4, max(1, len(home) // 2))
            back[home[0]], home = home[:count], home[count:]
        return list(out.values()), list(back.values())

    def wait_pool(self, pools, n):
        amount = self.inbox.at[pl.ds(0, len(pools[n]))]
        pltpu.make_async_copy(amount, amount, self.recv.at[n]).wait()

    def hops(self, offset):
        return sum(min(i, n - i) for i, n in zip(offset, self.g.sizes))

    def next_to(self):
        return [o for o in self.g.slots if self.hops(o) == 1]

    def piece(self, slot, p):
        size = self.rows // PIECES
        return pl.ds(self.pos[slot] * self.rows + p * size, size)

    def onward(self, o, p):
        return [k for k, (_, q, r, _) in enumerate(self.out_route) if r == o and q == p]

    def inward(self, o, p):
        parts = [(t, k) for k, (_, q, r, t) in enumerate(self.back_route) if r == o and q == p]
        return [k for _, k in sorted(parts)]

    def start_gather(self, hops):
        for k, (o, _, r, _) in enumerate(self.out_route):
            if r == self.home and self.hops(o) == hops:
                self.gather[k].start()

    def arrive(self, k):
        o, p, _, _ = self.out_route[k]
        pool = [n for n, ks in enumerate(self.out_pools) if k in ks][0]
        self.landed.add(k)
        if not self.landed.issuperset(self.out_pools[pool]):
            return
        self.wait_pool(self.out_pools, pool)
        for j in self.onward(o, p):
            assert self.hops(self.g.sub(self.out_route[j][0], o)) <= 2
            self.gather[j].start()

    def keep_sum(self, position, row):
        slot = self.g.slots[position]
        self.mine[pl.ds(self.g.index(slot), 1), 0 : self.rows] = row

    def start_sums(self):
        for copy in self.exchange:
            copy.start()

    def total(self):
        pltpu.make_async_copy(self.sums, self.sums, self.sum_recv.at[0]).wait()
        total = self.mine[...]
        for k in range(len(self.exchange)):
            total = total + self.sums[k]
        return total

    def send_ready(self, slots):
        for k, (o, p, _, _) in enumerate(self.back_route):
            if self.g.neg(o) in slots and not self.inward(o, p):
                self.reduce[k].start()

    def stops(self):
        parts = [(self.inward(o, p), k) for k, (o, p, _, _) in enumerate(self.back_route)]
        return [(self.back_route[inward[-1]][3], k) for inward, k in parts if inward]

    def pass_on(self, k):
        o, p, _, _ = self.back_route[k]
        where = self.piece(self.g.neg(o), p)
        total = self.own[where, :]
        parts = self.inward(o, p)
        self.wait_pool(self.back_pools, [n for n, ks in enumerate(self.back_pools) if parts[0] in ks][0])
        for j in parts:
            total = total + self.inbox[j].astype(F32)
        self.out[where, :] = total.astype(BF16)
        self.reduce[k].start()

    def home_parts(self):
        return [(t, k) for k, (_, _, r, t) in enumerate(self.back_route) if r == self.home]

    def home_pools(self):
        when = dict((k, t) for t, k in self.home_parts())
        return [(max(when[k] for k in ks), n) for n, ks in enumerate(self.back_pools) if ks[0] in when]

    def add_home(self, n, grad):
        size = self.rows // PIECES
        self.wait_pool(self.back_pools, n)
        for p in range(PIECES):
            parts = [k for k in self.back_pools[n] if self.back_route[k][1] == p]
            if parts:
                here = slice(p * size, (p + 1) * size)
                grad[here, :] = sum((self.inbox[k].astype(F32) for k in parts), grad[here, :])

    def wait_sends(self, n):
        amount = (self.inbox, self.sums)[n]
        pltpu.make_async_copy(amount, amount, self.send.at[n]).wait()


def kernel(
    side,
    image_hbm, text_hbm,
    image_loss, text_loss, image_grad, text_grad,
    image_raw, text_raw, images, texts, power, pull,
    row_mine, row_in, col_mine, col_in, row_tot, col_tot, row_all, col_all,
    image_own, text_own, image_out, text_out, image_box, text_box,
    around, *sems,
):
    lane, block, unit = lax.axis_index("lane"), lax.axis_index("block"), lax.axis_index("unit")
    z, y = block // side, lax.rem(block, side)
    rows = image_raw.shape[0]
    image_count = row_mine.shape[0]
    sizes = (IMAGE_GROUPS, TEXT_GROUPS)
    first = [[sum(s[:g]) for g in range(len(s) + 1)] for s in sizes]
    group_of = [[g for g, n in enumerate(s) for _ in range(n)] for s in sizes]

    loads = [
        pltpu.make_async_copy(image_hbm, image_raw, sems[0].at[0]),
        pltpu.make_async_copy(text_hbm, text_raw, sems[3].at[0]),
    ]
    for load in loads:
        load.start()
    barrier = pltpu.get_barrier_semaphore()

    def sides(plan):
        line = Group(plan[0][0], (image_count,), (z,), lambda k: {"block": k * side + y})
        plane = Group(plan[1][0], (side, side), (y, lane), lambda k, j: {"block": z * side + k, "lane": j})
        return (
            Side(line, group_of[0], plan[0], rows, images, row_in, row_mine, image_own, image_out, image_box, sems[:3]),
            Side(plane, group_of[1], plan[1], rows, texts, col_in, col_mine, text_own, text_out, text_box, sems[3:]),
        )

    def some(s, gs):
        start, end = first[s][gs[0]] * rows, first[s][gs[-1] + 1] * rows
        return pl.ds(start, end - start)

    def run(plan):
        image, text = sides(plan)
        for part in (image, text):
            for o in part.next_to():
                pl.semaphore_signal(barrier, inc=1, device_id=part.g.device(o))
        with jax.named_scope("load"):
            loads[1].wait()
            texts[0:rows, :] = unit_rows(text_raw[...])
            loads[0].wait()
            images[0:rows, :] = unit_rows(image_raw[...])
        with jax.named_scope("barrier"):
            pl.semaphore_wait(barrier, len(image.next_to()) + len(text.next_to()))
        for part in (image, text):
            for o in part.next_to():
                pl.semaphore_signal(around, inc=1, device_id=part.g.device(o))
        text.start_gather(1)
        image.start_gather(1)

        with jax.named_scope("around"):
            pl.semaphore_wait(around, len(image.next_to()) + len(text.next_to()))
        image.start_gather(2)
        text.start_gather(2)

        pair = 12.0 * lax.dot_general(images[0:rows, :], texts[0:rows, :], NT, preferred_element_type=F32)
        eye = lax.broadcasted_iota(jnp.int32, (rows, rows), 0) == lax.broadcasted_iota(jnp.int32, (rows, rows), 1)
        matched = jnp.sum(jnp.where(eye, pair, 0.0), axis=0, keepdims=True)

        row_sums, col_sums = [0.0] * len(IMAGE_GROUPS), [0.0] * len(TEXT_GROUPS)

        def powers(hs, gs):
            here, there = some(0, hs), some(1, gs)
            logit = lax.dot_general(images[here, :], texts[there, :], NT, preferred_element_type=F32)
            p = jnp.exp2((12.0 * LOG2E) * logit)
            power[here, there] = p
            lanes = sum(p[:, k : k + 128] for k in range(0, p.shape[1], 128))
            for s, groups, sums in ((0, hs, row_sums), (1, gs, col_sums)):
                start = 0
                for g in groups:
                    end = start + sizes[s][g] * rows
                    sums[g] += jnp.sum(p[:, start:end], axis=0, keepdims=True) if s else lanes[start:end]
                    start = end

        def keep_sums(s, g):
            part, row = (image, text)[s], (row_sums, col_sums)[s][g]
            row = row if s else jnp.sum(jnp.transpose(row), axis=0, keepdims=True)
            for k in range(sizes[s][g]):
                part.keep_sum(first[s][g] + k, row[:, k * rows : (k + 1) * rows])

        waits = sorted(
            (t, s, k) for s, part in enumerate((image, text)) for k, (_, _, _, t) in enumerate(part.out_route)
        )
        missing = {(s, g): set() for s in (0, 1) for g in range(len(sizes[s]))}
        for s, part in enumerate((image, text)):
            for k, (o, _, _, _) in enumerate(part.out_route):
                missing[(s, group_of[s][part.pos[part.g.neg(o)]])].add(k)
        todo = {(h, g) for h in range(len(IMAGE_GROUPS)) for g in range(len(TEXT_GROUPS))}
        for _, s, k in waits:
            part = (image, text)[s]
            with jax.named_scope(f"arrive_{'it'[s]}{k:02d}"):
                part.arrive(k)
            missing[(s, group_of[s][part.pos[part.g.neg(part.out_route[k][0])]])].discard(k)
            ready = {(h, g) for h, g in todo if not missing[(0, h)] and not missing[(1, g)]}
            todo -= ready
            for hs, gs in rectangles(ready):
                with jax.named_scope(f"pow{hs[0]}{gs[0]}"):
                    powers(hs, gs)
            for g in sorted({g for _, g in ready} - {g for _, g in todo}):
                keep_sums(1, g)

        with jax.named_scope("sums_out"):
            text.start_sums()
            for h in range(len(IMAGE_GROUPS)):
                keep_sums(0, h)
            image.start_sums()

        def inverse(part, totals, lines):
            totals[...] = 1.0 / part.total()
            for k, slot in enumerate(part.g.slots):
                lines[:, k * rows : (k + 1) * rows] = totals[pl.ds(part.g.index(slot), 1), 0:rows]

        with jax.named_scope("sums_in"):
            inverse(image, row_tot, row_all)
            row_inv = row_all[...]
            row_inv_up = upright(row_inv)
            inverse(text, col_tot, col_all)
            col_inv = col_all[...]

        def scale(start, end):
            values = power[:, start:end] * (row_inv_up + col_inv[:, start:end])
            if start == 0:
                ids = [lax.broadcasted_iota(jnp.int32, values.shape, d) for d in (0, 1)]
                values = values - jnp.where((ids[0] == ids[1]) & (ids[0] < rows), 2.0, 0.0)
            pull[:, start:end] = values.astype(BF16)

        image.wait_sends(0)
        text.wait_sends(0)
        scaled = pull.shape[1]
        for s, first_slot, end_slot in BACK_ORDER:
            start, end = first_slot * rows, end_slot * rows
            part, own, out = ((image, image_own, image_out), (text, text_own, text_out))[s]
            with jax.named_scope(f"g{'it'[s]}{first_slot}"):
                if scaled > s * start:
                    scale(s * start, scaled)
                    scaled = s * start
                if s == 0:
                    grad = jnp.dot(pull[start:end, :], texts[...], preferred_element_type=F32)
                else:
                    grad = lax.dot_general(pull[:, start:end], images[...], TN, preferred_element_type=F32)
                own[start:end, :] = grad
                out[start:end, :] = grad.astype(BF16)
                part.send_ready(part.g.slots[first_slot:end_slot])
        image_loss[...] = -jnp.log(row_inv[:, 0:rows]) - matched
        text_loss[...] = -jnp.log(col_inv[:, 0:rows]) - matched
        for _, s, k in sorted((t, s, k) for s, part in enumerate((image, text)) for t, k in part.stops()):
            part = (image, text)[s]
            with jax.named_scope(f"pass_{'it'[s]}{k:02d}"):
                part.pass_on(k)
        image_grad[...] = image_own[0:rows, :]
        text_grad[...] = text_own[0:rows, :]
        with jax.named_scope("out"):
            for _, s, k in sorted((t, s, k) for s, part in enumerate((image, text)) for t, k in part.home_pools()):
                (image, text)[s].add_home(k, (image_grad, text_grad)[s])
        with jax.named_scope("wait_sends"):
            for part in (image, text):
                part.wait_sends(0)
                part.wait_sends(1)

    if len(PLANS) == 1:
        run(PLANS[0])
    else:
        for k, plan in enumerate(PLANS):
            pl.when(unit == k)(functools.partial(run, plan))


def place(*refs):
    sem = refs[-1]
    copies = [
        pltpu.make_async_copy(refs[i], refs[i + 4], sem.at[i]) for i in (2, 3, 0, 1)
    ]
    for copy in copies:
        copy.start()
    for copy in copies:
        copy.wait()


def solution(mesh):
    side = mesh.shape["lane"]

    def body(image_rows, text_rows):
        rows, width = image_rows.shape
        nz, npl = mesh.shape["block"] // side, side * side
        images_n, texts_n = nz * rows, npl * rows
        routes = [len(route[0]) for route in PLANS[0]]
        semaphores = (RECV_SEMS[0], RECV_SEMS[1])
        scratch = [
            pltpu.VMEM((rows, width), BF16),
            pltpu.VMEM((rows, width), BF16),
            pltpu.VMEM((images_n, width), BF16),
            pltpu.VMEM((texts_n, width), BF16),
            pltpu.VMEM((images_n, texts_n), F32),
            pltpu.VMEM((images_n, texts_n), BF16),
            pltpu.VMEM((nz, 128), F32),
            pltpu.VMEM((nz - 1, nz, 128), F32),
            pltpu.VMEM((npl, 128), F32),
            pltpu.VMEM((npl - 1, npl, 128), F32),
            pltpu.VMEM((nz, 128), F32),
            pltpu.VMEM((npl, 128), F32),
            pltpu.VMEM((1, images_n), F32),
            pltpu.VMEM((1, texts_n), F32),
            pltpu.VMEM((images_n, width), F32),
            pltpu.VMEM((texts_n, width), F32),
            pltpu.VMEM((images_n, width), BF16),
            pltpu.VMEM((texts_n, width), BF16),
            pltpu.VMEM((routes[0], rows // PIECES, width), BF16),
            pltpu.VMEM((routes[1], rows // PIECES, width), BF16),
        ]
        scratch.append(pltpu.SemaphoreType.REGULAR)
        for count in semaphores:
            scratch += [pltpu.SemaphoreType.DMA((n,)) for n in (2, count, 1)]
        results = pl.pallas_call(
            functools.partial(kernel, side),
            out_shape=(
                jax.ShapeDtypeStruct((1, rows), F32),
                jax.ShapeDtypeStruct((1, rows), F32),
                jax.ShapeDtypeStruct((rows, width), F32),
                jax.ShapeDtypeStruct((rows, width), F32),
            ),
            in_specs=[pl.BlockSpec(memory_space=pltpu.HBM)] * 2,
            out_specs=[pl.BlockSpec(memory_space=pltpu.VMEM)] * 4,
            scratch_shapes=scratch,
            compiler_params=pltpu.CompilerParams(
                collective_id=0, has_side_effects=True, vmem_limit_bytes=40 * 2**20
            ),
        )(*(pltpu.with_memory_space_constraint(x, pltpu.HBM) for x in (image_rows, text_rows)))
        image_loss, text_loss, image_grad, text_grad = pl.pallas_call(
            place,
            out_shape=tuple(jax.ShapeDtypeStruct(r.shape, r.dtype) for r in results),
            in_specs=[pl.BlockSpec(memory_space=pltpu.VMEM)] * 4,
            out_specs=[pl.BlockSpec(memory_space=pl.ANY)] * 4,
            scratch_shapes=[pltpu.SemaphoreType.DMA((4,))],
            compiler_params=pltpu.CompilerParams(vmem_limit_bytes=4 * rows * width * 8),
        )(*results)
        return (image_loss.reshape(rows), text_loss.reshape(rows), image_grad, text_grad)

    rows_spec = P(("unit", "block", "lane"), None)
    flat_spec = P(("unit", "block", "lane"))
    return jax.shard_map(
        body,
        mesh=mesh,
        in_specs=(rows_spec, rows_spec),
        out_specs=(flat_spec, flat_spec, rows_spec, rows_spec),
        check_vma=False,
    )
```
